32 devices in a mesh: dp: 1 (over z), cp: 4 (over y), tp: 8 (over x, core).
Axes of the slice: x: 4, y: 4, z: 1, core: 2. Of those that a mesh axis runs over, the one named last changes fastest.
The devices are a block of a 4x4x8 slice.
Arguments:
- x: bfloat16 [8192, 2048], P(('dp', 'cp', 'tp'))
- idx: int32 [8192, 2], P(('dp', 'cp', 'tp'))
- gates: float32 [8192, 2], P(('dp', 'cp', 'tp'))
- wq: bfloat16 [2048, 2048], P(None, 'tp')
- wk: bfloat16 [2048, 2048], P(None, 'tp')
- wv: bfloat16 [2048, 2048], P(None, 'tp')
- wo: bfloat16 [2048, 2048], P('tp')
- w1g: bfloat16 [32, 2048, 1024], P(('cp', 'tp'))
- w1u: bfloat16 [32, 2048, 1024], P(('cp', 'tp'))
- w2: bfloat16 [32, 1024, 2048], P(('cp', 'tp'))
Outputs:
- output: bfloat16 [8192, 2048], P(('dp', 'cp', 'tp'))
All inputs are finite; a program needn't handle non-finite values.
Results may differ from the reference program's by a relative error of at most 0.010004.
Values are sent between devices in bfloat16 or wider.
A program may use at most 768 MiB of HBM per device.

```python
import math
import jax
import jax.numpy as jnp
from jax import lax

H = 2048
FF = 1024
HEADS = 16
KV_HEADS = 16
HEAD = 128
S = 8192
CP = 4
TP = 8
TOP = 2
QBLK = 512

E = CP * TP
T = S // E
CAP = 4 * T // E
M = 2 * T // E


def seg_positions():
    i = jnp.arange(S, dtype=jnp.int32)
    seg = S // (2 * CP)
    b = i // seg
    r = b // 2
    s_id = jnp.where(b % 2 == 0, r, 2 * CP - 1 - r)
    return s_id * seg + i % seg


def source_routing(key, sigma, counts):
    ends = jnp.cumsum(counts)
    labels = sigma[jnp.searchsorted(ends, jnp.arange(2 * T, dtype=jnp.int32), side='right')]
    perm = jax.random.permutation(key, T)
    return jnp.stack([labels[perm], labels[perm + T]], axis=1).astype(jnp.int32)


def setup_inputs(seed: int = 0, part: int = 0) -> dict:
    key = jax.random.key(seed)
    ks = jax.random.split(key, 7)
    kx = jax.random.split(jax.random.fold_in(key, part), 4)
    a = math.log(S / 16.0) ** 0.25

    def nrm(k, shape, scale):
        return (jax.random.normal(k, shape, jnp.float32) * scale).astype(jnp.bfloat16)

    wq = nrm(ks[0], (H, HEADS * HEAD), a / math.sqrt(H))
    wk = nrm(ks[1], (H, KV_HEADS * HEAD), a / math.sqrt(H))
    wv = nrm(ks[2], (H, KV_HEADS * HEAD), 1.0 / math.sqrt(H))
    wo = nrm(ks[3], (HEADS * HEAD, H), 1.0 / math.sqrt(HEADS * HEAD))
    w1g = nrm(ks[4], (E, H, FF), 1.0 / math.sqrt(H))
    w1u = nrm(ks[5], (E, H, FF), 1.0 / math.sqrt(H))
    w2 = nrm(ks[6], (E, FF, H), 1.5 / math.sqrt(FF))
    x = nrm(kx[0], (S, H), 1.0)
    sigmas = jax.vmap(lambda kk: jax.random.permutation(kk, E))(jax.random.split(kx[1], E))
    counts = jnp.full((E,), M, jnp.int32)
    idx = jax.vmap(lambda kk, sg: source_routing(kk, sg, counts))(jax.random.split(kx[2], E), sigmas)
    idx = idx.reshape(S, TOP)
    gates = jax.random.uniform(kx[3], (S, TOP), jnp.float32, 0.3, 0.7)
    return {'x': x, 'idx': idx, 'gates': gates, 'wq': wq, 'wk': wk, 'wv': wv, 'wo': wo, 'w1g': w1g, 'w1u': w1u, 'w2': w2}


def reference(x, idx, gates, wq, wk, wv, wo, w1g, w1u, w2):
    pos = seg_positions()
    g = HEADS // KV_HEADS
    q = jnp.dot(x, wq, preferred_element_type=jnp.float32).astype(jnp.bfloat16)
    k = jnp.dot(x, wk, preferred_element_type=jnp.float32).astype(jnp.bfloat16)
    v = jnp.dot(x, wv, preferred_element_type=jnp.float32).astype(jnp.bfloat16)
    qh = q.reshape(S, HEADS, HEAD).transpose(1, 0, 2)
    kh = jnp.repeat(k.reshape(S, KV_HEADS, HEAD).transpose(1, 0, 2), g, axis=0)
    vh = jnp.repeat(v.reshape(S, KV_HEADS, HEAD).transpose(1, 0, 2), g, axis=0)
    scale = HEAD ** -0.5
    nb = S // QBLK

    def head(args):
        qa, ka, va = args

        def block(bargs):
            qb, pb = bargs
            s = jnp.dot(qb, ka.T, preferred_element_type=jnp.float32) * scale
            mask = pos[None, :] <= pb[:, None]
            s = jnp.where(mask, s, -1e30)
            m = jnp.max(s, axis=-1, keepdims=True)
            w = jnp.where(mask, jnp.exp(s - m), 0.0)
            l = jnp.sum(w, axis=-1, keepdims=True)
            ob = jnp.dot(w.astype(jnp.bfloat16), va, preferred_element_type=jnp.float32)
            return ob / l

        out = lax.map(block, (qa.reshape(nb, QBLK, HEAD), pos.reshape(nb, QBLK)))
        return out.reshape(S, HEAD)

    o = lax.map(head, (qh, kh, vh))
    o = o.transpose(1, 0, 2).reshape(S, HEADS * HEAD).astype(jnp.bfloat16)
    att = jnp.dot(o, wo, preferred_element_type=jnp.float32)
    h = (x.astype(jnp.float32) + att).astype(jnp.bfloat16)

    ea = idx.reshape(-1)
    tok = jnp.arange(S * TOP) // TOP
    onehot = (ea[:, None] == jnp.arange(E)[None, :]).astype(jnp.int32)
    slot = jnp.take_along_axis(jnp.cumsum(onehot, axis=0), ea[:, None], axis=1)[:, 0] - 1
    ct = E * CAP
    buf = jnp.zeros((E, ct, H), jnp.bfloat16).at[ea, slot].set(h[tok])

    def expert(args):
        rows, wg, wu, wd = args
        gg = jnp.dot(rows, wg, preferred_element_type=jnp.float32)
        uu = jnp.dot(rows, wu, preferred_element_type=jnp.float32)
        act = (jax.nn.silu(gg) * uu).astype(jnp.bfloat16)
        return jnp.dot(act, wd, preferred_element_type=jnp.float32).astype(jnp.bfloat16)

    z = lax.map(expert, (buf, w1g, w1u, w2))
    zt = z[ea, slot].astype(jnp.float32).reshape(S, TOP, H)
    y = h.astype(jnp.float32) + jnp.sum(gates[:, :, None] * zt, axis=1)
    return y.astype(jnp.bfloat16)
```

```python
import functools
import math

import jax
import jax.numpy as jnp
from jax import lax
from jax.experimental import pallas as pl
from jax.experimental.pallas import tpu as pltpu
from jax.sharding import PartitionSpec as P

HEAD = 128
MESH = pl.DeviceIdType.MESH
VMEM = pltpu.VMEM
DMA = pltpu.SemaphoreType.DMA
BF16 = jnp.bfloat16
F32 = jnp.float32


def spec(space):
    return pl.BlockSpec(memory_space=space)


def remote(src, dst, ssem, rsem, dev):
    return pltpu.make_async_remote_copy(src_ref=src, dst_ref=dst, send_sem=ssem, recv_sem=rsem, device_id=dev, device_id_type=MESH)


def barrier_with(devs):
    b = pltpu.get_barrier_semaphore()
    for d in devs:
        pl.semaphore_signal(b, inc=1, device_id=d, device_id_type=MESH)
    pl.semaphore_wait(b, len(devs))


def place(c, chip, core, cp):
    high = chip // 2
    seg = c * (1 - high) + (2 * cp - 1 - c) * high
    return seg * 4 + (chip % 2) * 2 + core


def qkv_kernel(cp, nx, x_ref, wq_ref, wk_ref, wv_ref, kvq, wsib, xb, stage, wss, wrs, xss, xrs, ass, ars, rss, rrs, ls):
    c = lax.axis_index('cp')
    t = lax.axis_index('tp')
    i, k = t // 2, t % 2
    T = x_ref.shape[0]
    half = T // 2
    sib = {'cp': c, 'tp': i * 2 + 1 - k}
    right = {'cp': c, 'tp': ((i + 1) % nx) * 2 + k}
    left = {'cp': c, 'tp': ((i + nx - 1) % nx) * 2 + k}
    peer = [{'cp': (c + d) % cp, 'tp': t} for d in range(cp)]
    barrier_with([sib, right, left] + peer[1:])
    lo, hi = pl.ds(0, half), pl.ds(half, half)
    full = pl.ds(0, T)

    def xcopy(n, src, slot, rows, dev):
        return remote(src.at[rows], xb.at[slot, rows], xss.at[n], xrs.at[n], dev)

    sends = [
        xcopy(0, x_ref, 0, lo, right), xcopy(1, x_ref, 1, hi, left),
        xcopy(2, x_ref, 0, hi, right), xcopy(3, x_ref, 1, lo, left),
    ]
    own_w = [wq_ref, wk_ref, wv_ref]
    wsend = [remote(own_w[n], wsib.at[n], wss.at[n], wrs.at[n], sib) for n in range(3)]
    for s in (sends[0], sends[1], *wsend, sends[2], sends[3]):
        s.start()

    pend = list(sends) + wsend
    arrive = []

    units = [(0, full), (nx - 1, lo), (1, hi), (nx - 1, hi), (1, lo), (2, lo), (2, hi)]

    def compute(u, src, rows):
        xv = src[rows, :]
        for w in range(2):
            if u == 0 and w == 1:
                for s in wsend:
                    s.wait_recv()
            for n in range(3):
                wref = own_w[n] if w == 0 else wsib.at[n]
                r = jnp.dot(xv, wref[...], preferred_element_type=F32).astype(BF16)
                kk = k if w == 0 else 1 - k
                for m in range(2):
                    stage[u, 2 * kk + m, n, rows, :] = r[:, m * HEAD:(m + 1) * HEAD]

    def block_of(u, d):
        dj, _ = units[u]
        return place((c + cp - d) % cp, (i + dj) % nx, k, cp)

    def send(u):
        rows = units[u][1]
        b = block_of(u, 0)
        for d in range(1, cp):
            cps = remote(stage.at[u, (c + d) % cp, :, rows], kvq.at[b, :, rows], ass.at[u, d], ars.at[u, d], peer[d])
            cps.start()
            pend.append(cps)
        lc = pltpu.make_async_copy(stage.at[u, c, :, rows], kvq.at[b, :, rows], ls.at[u])
        lc.start()
        locs.append(lc)
        relay(u, 0, stage.at[u, c, pl.ds(1, 2), rows])

    def relay(u, d, src):
        rows = units[u][1]
        b = block_of(u, d)
        cps = remote(src, kvq.at[b, pl.ds(1, 2), rows], rss.at[u, d], rrs.at[u, d], sib)
        cps.start()
        pend.append(cps)
        arrive.append((u, d))

    def pass_on(u):
        rows = units[u][1]
        for d in range(1, cp):
            b = block_of(u, d)
            remote(stage.at[u, 0, :, rows], kvq.at[b, :, rows], ass.at[u, d], ars.at[u, d], peer[d]).wait_recv()
            relay(u, d, kvq.at[b, pl.ds(1, 2), rows])

    locs = []
    compute(0, x_ref, full)
    send(0)
    sends[0].wait_recv()
    f = xcopy(4, xb.at[0], 2, lo, right)
    f.start()
    g = xcopy(5, xb.at[1], 2, hi, left)
    sends[1].wait_recv()
    g.start()
    pend += [f, g]
    compute(1, xb.at[0], lo)
    send(1)
    compute(2, xb.at[1], hi)
    send(2)
    pass_on(0)
    sends[2].wait_recv()
    compute(3, xb.at[0], hi)
    send(3)
    sends[3].wait_recv()
    compute(4, xb.at[1], lo)
    send(4)
    pass_on(1)
    pass_on(2)
    f.wait_recv()
    compute(5, xb.at[2], lo)
    send(5)
    g.wait_recv()
    compute(6, xb.at[2], hi)
    send(6)
    for u in range(3, 7):
        pass_on(u)
    for u, d in arrive:
        rows = units[u][1]
        b = block_of(u, d) + 1 - 2 * k
        remote(stage.at[u, 0, pl.ds(1, 2), rows], kvq.at[b, pl.ds(1, 2), rows], rss.at[u, d], rrs.at[u, d], sib).wait_recv()
    for lc in locs:
        lc.wait()
    for s in pend:
        s.wait_send()


def attn_kernel(cp, nx, kvq, wo_ref, x_ref, h_ref, vt, wof, ostage, obuf, wss, wrs, oss, ors, ls):
    c = lax.axis_index('cp')
    t = lax.axis_index('tp')
    i, k = t // 2, t % 2
    T, H = x_ref.shape
    R = wo_ref.shape[0]
    nch = kvq.shape[0] // 2
    sib = {'cp': c, 'tp': i * 2 + 1 - k}
    ri, li, oi = (i + 1) % nx, (i + nx - 1) % nx, (i + 2) % nx
    right = {'cp': c, 'tp': ri * 2 + k}
    left = {'cp': c, 'tp': li * 2 + k}
    offs = [(di, dc) for di in range(nx) for dc in range(cp)]

    def dev(di, dc):
        return {'cp': (c + dc) % cp, 'tp': ((i + di) % nx) * 2 + k}

    barrier_with([sib] + [dev(di, dc) for di, dc in offs[1:]])
    half = R // 2
    lo, hi, full = pl.ds(0, half), pl.ds(half, half), pl.ds(0, R)
    own = t

    def wcopy(n, src, chip, core, rows, to):
        return remote(src, wof.at[chip * 2 + core, rows], wss.at[n], wrs.at[n], to)

    w0 = wcopy(0, wo_ref.at[lo], i, k, lo, right)
    w1 = wcopy(1, wo_ref.at[hi], i, k, hi, left)
    w2 = wcopy(2, wo_ref.at[hi], i, k, hi, right)
    w3 = wcopy(3, wo_ref.at[lo], i, k, lo, left)
    w6 = wcopy(6, wo_ref, i, k, full, sib)
    for w in (w0, w1, w2, w3, w6):
        w.start()
    wl = pltpu.make_async_copy(wo_ref, wof.at[t], ls.at[0])
    wl.start()
    w4 = wcopy(4, wof.at[li * 2 + k, lo], li, k, lo, right)
    w5 = wcopy(5, wof.at[ri * 2 + k, hi], ri, k, hi, left)
    w7 = wcopy(7, wof.at[li * 2 + k], li, k, full, sib)
    w8 = wcopy(8, wof.at[ri * 2 + k], ri, k, full, sib)
    w9 = wcopy(9, wof.at[oi * 2 + k], oi, k, full, sib)

    @pl.loop(0, nch)
    def _(m):
        v = kvq[pl.ds(2 * m, 2), 2].reshape(2 * T, HEAD)
        vt[m] = v.astype(F32).T.astype(BF16)

    scale = HEAD ** -0.5 * math.log2(math.e)

    def step(q, m, mask, carry):
        mo, l, acc = carry
        kb = kvq[pl.ds(2 * m, 2), 1].reshape(2 * T, HEAD)
        s = lax.dot_general(kb, q, (((1,), (1,)), ((), ())), preferred_element_type=F32)
        if mask is not None:
            s = jnp.where(mask, s, -jnp.inf)
        mn = jnp.maximum(mo, jnp.max(s, axis=0, keepdims=True))
        w = jnp.exp2((s - mn) * scale)
        a = jnp.exp2((mo - mn) * scale)
        l = l * a + jnp.sum(w, axis=0, keepdims=True)
        acc = acc * a + jnp.dot(vt[m], w.astype(BF16), preferred_element_type=F32)
        return mn, l, acc

    rows_i = lax.broadcasted_iota(jnp.int32, (2 * T, T), 0)
    cols_i = lax.broadcasted_iota(jnp.int32, (2 * T, T), 1)
    order = offs[1:] + offs[:1]

    def attend(n):
        di, dc = n // cp, n % cp
        pb = place((c + dc) % cp, (i + di) % nx, k, cp)
        q = kvq[pb, 0]
        m = pb // 2
        carry = (jnp.full((1, T), -jnp.inf, F32), jnp.zeros((1, T), F32), jnp.zeros((HEAD, T), F32))
        carry = lax.fori_loop(0, m, lambda j, cr: step(q, j, None, cr), carry)
        mo, l, acc = step(q, m, rows_i <= cols_i + k * T, carry)
        ostage[n] = (acc / l).T.astype(BF16)

    head = i * cp + c
    col = pl.ds((c % 2) * HEAD, HEAD)

    def osend(n, to):
        return remote(ostage.at[n], obuf.at[i * 2 + c // 2, :, col], oss.at[n], ors.at[n], to)

    nall = nx * cp

    def run(a, b):
        @pl.loop(a, b)
        def _(n):
            attend(n)
            osend(n, {'cp': (c + n % cp) % cp, 'tp': ((i + n // cp) % nx) * 2 + k}).start()

    run(1, 6)
    w0.wait_recv()
    w4.start()
    w1.wait_recv()
    w5.start()
    run(6, 11)
    w2.wait_recv()
    w7.start()
    w3.wait_recv()
    w8.start()
    run(11, nall)
    attend(0)
    lo_c = pltpu.make_async_copy(ostage.at[0], obuf.at[i * 2 + c // 2, :, col], ls.at[1])
    lo_c.start()
    w4.wait_recv()
    w5.wait_recv()
    w9.start()
    wl.wait()
    for w in (w6, w7, w8, w9):
        w.wait_recv()
    lo_c.wait()

    @pl.loop(1, nall)
    def _(n):
        osend(n, {'cp': (c + n % cp) % cp, 'tp': ((i + n // cp) % nx) * 2 + k}).wait_recv()

    nt = wof.shape[0]
    cw = min(512, H)
    for j in range(H // cw):
        cs = slice(j * cw, (j + 1) * cw)
        a = jnp.dot(obuf[0], wof[0, :, cs], preferred_element_type=F32)
        for tt in range(1, nt):
            a += jnp.dot(obuf[tt], wof[tt, :, cs], preferred_element_type=F32)
        h_ref[:, cs] = (x_ref[:, cs].astype(F32) + a).astype(BF16)

    for w in (w0, w1, w2, w3, w4, w5, w6, w7, w8, w9):
        w.wait_send()

    @pl.loop(1, nall)
    def _(n):
        osend(n, {'cp': (c + n % cp) % cp, 'tp': ((i + n // cp) % nx) * 2 + k}).wait_send()


def moe_kernel(cp, tp, cap, h_ref, p_ref, g0_ref, g1_ref, gates_ref, wg_hbm, wu_hbm, wd_hbm, y_ref,
               sendb, recvb, zb, back, wg, wu, wd, acc0, acc1, wsem, dss, drs, bss, brs):
    c = lax.axis_index('cp')
    t = lax.axis_index('tp')
    ne = cp * tp
    T, H = h_ref.shape
    grp = 4
    ng = ne // grp
    wc = [pltpu.make_async_copy(a.at[0], b, wsem.at[n]) for n, (a, b) in enumerate(((wg_hbm, wg), (wu_hbm, wu), (wd_hbm, wd)))]
    for w in wc:
        w.start()

    def fwd(d):
        return {'cp': (c + d // tp) % cp, 'tp': (t + d % tp) % tp}

    def bwd(d):
        return {'cp': (c + cp - d // tp) % cp, 'tp': (t + tp - d % tp) % tp}

    b = pltpu.get_barrier_semaphore()

    @pl.loop(1, ne)
    def _(d):
        pl.semaphore_signal(b, inc=1, device_id=fwd(d), device_id_type=MESH)

    def pack(g):
        rows = p_ref[pl.ds(g * grp * cap, grp * cap), :]
        r = jnp.dot(rows, h_ref[...], preferred_element_type=F32).astype(BF16)
        sendb[pl.ds(g * grp, grp)] = r.reshape(grp, cap, H)

    def disp(d):
        return remote(sendb.at[d], recvb.at[d], dss.at[d], drs.at[d], fwd(d))

    def ret(d):
        return remote(zb.at[d], back.at[d], bss.at[d], brs.at[d], bwd(d))

    pack(0)
    recvb[0] = sendb[0]
    pl.semaphore_wait(b, ne - 1)
    for d in range(1, grp):
        disp(d).start()

    @pl.loop(1, ng)
    def _(g):
        pack(g)
        for j in range(grp):
            disp(g * grp + j).start()

    for w in wc:
        w.wait()

    def ffn(g):
        rows = recvb[pl.ds(g * grp, grp)].reshape(grp * cap, H)
        gg = jnp.dot(rows, wg[...], preferred_element_type=F32)
        uu = jnp.dot(rows, wu[...], preferred_element_type=F32)
        act = (gg * jax.nn.sigmoid(gg) * uu).astype(BF16)
        z = jnp.dot(act, wd[...], preferred_element_type=F32).astype(BF16)
        zb[pl.ds(g * grp, grp)] = z.reshape(grp, cap, H)

    def combine(g):
        zz = back[pl.ds(g * grp, grp)].reshape(grp * cap, H)
        cols = pl.ds(pl.multiple_of(g * grp * cap, grp * cap), grp * cap)
        return (jnp.dot(g0_ref[:, cols], zz, preferred_element_type=F32),
                jnp.dot(g1_ref[:, cols], zz, preferred_element_type=F32))

    for d in range(1, grp):
        disp(d).wait_recv()
    ffn(0)
    back[0] = zb[0]
    for d in range(1, grp):
        ret(d).start()

    @pl.loop(1, ng)
    def _(g):
        for j in range(grp):
            disp(g * grp + j).wait_recv()
        ffn(g)
        for j in range(grp):
            ret(g * grp + j).start()

    for d in range(1, grp):
        ret(d).wait_recv()
    a, bb = combine(0)
    acc0[...] = a
    acc1[...] = bb

    @pl.loop(1, ng)
    def _(g):
        for j in range(grp):
            ret(g * grp + j).wait_recv()
        a, bb = combine(g)
        acc0[...] += a
        acc1[...] += bb

    y_ref[...] = (h_ref[...].astype(F32) + (gates_ref[:, 0:1] * acc0[...] + gates_ref[:, 1:2] * acc1[...])).astype(BF16)

    @pl.loop(1, ne)
    def _(d):
        disp(d).wait_send()
        ret(d).wait_send()


def params(cid):
    return pltpu.CompilerParams(collective_id=cid, has_side_effects=True, vmem_limit_bytes=60 * 1024 * 1024)


def attention(x, wq, wk, wv, wo, cp, tp):
    T, H = x.shape
    nx = tp // 2
    nb = cp * tp
    W = wq.shape[1]
    kvq = pl.pallas_call(
        functools.partial(qkv_kernel, cp, nx),
        out_shape=jax.ShapeDtypeStruct((nb, 3, T, HEAD), BF16),
        in_specs=[spec(VMEM)] * 4,
        out_specs=spec(VMEM),
        scratch_shapes=[
            VMEM((3, H, W), BF16), VMEM((3, T, H), BF16), VMEM((7, 4, 3, T, HEAD), BF16),
            DMA((3,)), DMA((3,)), DMA((6,)), DMA((6,)),
            DMA((7, cp)), DMA((7, cp)), DMA((7, cp)), DMA((7, cp)), DMA((7,)),
        ],
        compiler_params=params(0),
        name='qkv',
    )(x, wq, wk, wv)
    h = pl.pallas_call(
        functools.partial(attn_kernel, cp, nx),
        out_shape=jax.ShapeDtypeStruct((T, H), BF16),
        in_specs=[spec(VMEM)] * 3,
        out_specs=spec(VMEM),
        scratch_shapes=[
            VMEM((nb // 2, HEAD, 2 * T), BF16), VMEM((tp, wo.shape[0], H), BF16),
            VMEM((nx * cp, T, HEAD), BF16), VMEM((tp, T, 2 * HEAD), BF16),
            DMA((10,)), DMA((10,)), DMA((nx * cp,)), DMA((nx * cp,)), DMA((2,)),
        ],
        compiler_params=params(1),
        name='attn',
    )(kvq, wo, x)
    return h


def routing(idx, cp, tp, cap):
    ne = cp * tp
    T, kk = idx.shape
    c = lax.axis_index('cp')
    t = lax.axis_index('tp')
    rel = ((idx // tp - c + cp) % cp) * tp + (idx % tp - t + tp) % tp
    ea = rel.reshape(-1)
    onehot = (ea[:, None] == jnp.arange(ne)[None, :]).astype(jnp.int32)
    rank = jnp.cumsum(onehot, axis=0)
    slot = jnp.sum(onehot * rank, axis=1) - 1
    pos = (ea * cap + slot).reshape(T, kk)
    cols = jnp.arange(ne * cap, dtype=jnp.int32)
    g0 = pos[:, 0:1] == cols[None, :]
    g1 = pos[:, 1:2] == cols[None, :]
    p = (pos[:, 0][None, :] == cols[:, None]) | (pos[:, 1][None, :] == cols[:, None])
    return p.astype(BF16), g0.astype(BF16), g1.astype(BF16)


def experts(h, idx, gates, w1g, w1u, w2, cp, tp):
    T, H = h.shape
    F = w1g.shape[2]
    ne = cp * tp
    cap = 4 * T // ne
    p, g0, g1 = routing(idx, cp, tp, cap)
    return pl.pallas_call(
        functools.partial(moe_kernel, cp, tp, cap),
        out_shape=jax.ShapeDtypeStruct((T, H), BF16),
        in_specs=[spec(VMEM)] * 5 + [spec(pl.ANY)] * 3,
        out_specs=spec(VMEM),
        scratch_shapes=[VMEM((ne, cap, H), BF16)] * 4 + [
            VMEM((H, F), BF16), VMEM((H, F), BF16), VMEM((F, H), BF16), VMEM((T, H), F32), VMEM((T, H), F32),
            DMA((3,)), DMA((ne,)), DMA((ne,)), DMA((ne,)), DMA((ne,)),
        ],
        compiler_params=params(2),
        name='moe',
    )(h, p, g0, g1, gates, w1g, w1u, w2)


def solution(mesh):
    cp = mesh.shape['cp']
    tp = mesh.shape['tp']
    rows_spec = P(('dp', 'cp', 'tp'), None)
    exp_spec = P(('cp', 'tp'), None, None)

    def local(x, idx, gates, wq, wk, wv, wo, w1g, w1u, w2):
        h = attention(x, wq, wk, wv, wo, cp, tp)
        return experts(h, idx, gates, w1g, w1u, w2, cp, tp)

    return jax.shard_map(local, mesh=mesh, in_specs=(rows_spec, rows_spec, rows_spec, P(None, 'tp'), P(None, 'tp'), P(None, 'tp'), P('tp', None), exp_spec, exp_spec, exp_spec), out_specs=rows_spec, check_vma=False)
```

```python
import functools
import math

import jax
import jax.numpy as jnp
from jax import lax
from jax.experimental import pallas as pl
from jax.experimental.pallas import tpu as pltpu
from jax.sharding import PartitionSpec as P

HEAD = 128
MESH = pl.DeviceIdType.MESH
VMEM = pltpu.VMEM
DMA = pltpu.SemaphoreType.DMA
BF16 = jnp.bfloat16
F32 = jnp.float32


def spec(space):
    return pl.BlockSpec(memory_space=space)


def remote(src, dst, ssem, rsem, dev):
    return pltpu.make_async_remote_copy(src_ref=src, dst_ref=dst, send_sem=ssem, recv_sem=rsem, device_id=dev, device_id_type=MESH)


def barrier_with(devs):
    b = pltpu.get_barrier_semaphore()
    for d in devs:
        pl.semaphore_signal(b, inc=1, device_id=d, device_id_type=MESH)
    pl.semaphore_wait(b, len(devs))


def place(c, chip, core, cp):
    high = chip // 2
    seg = c * (1 - high) + (2 * cp - 1 - c) * high
    return seg * 4 + (chip % 2) * 2 + core


def qkv_kernel(cp, nx, x_ref, wq_ref, wk_ref, wv_ref, kvq, wsib, xb, stage, wss, wrs, xss, xrs, ass, ars, rss, rrs, ls):
    c = lax.axis_index('cp')
    t = lax.axis_index('tp')
    i, k = t // 2, t % 2
    T = x_ref.shape[0]
    half = T // 2
    sib = {'cp': c, 'tp': i * 2 + 1 - k}
    right = {'cp': c, 'tp': ((i + 1) % nx) * 2 + k}
    left = {'cp': c, 'tp': ((i + nx - 1) % nx) * 2 + k}
    peer = [{'cp': (c + d) % cp, 'tp': t} for d in range(cp)]
    barrier_with([sib, right, left] + peer[1:])
    lo, hi = pl.ds(0, half), pl.ds(half, half)
    full = pl.ds(0, T)

    def xcopy(n, src, slot, rows, dev):
        return remote(src.at[rows], xb.at[slot, rows], xss.at[n], xrs.at[n], dev)

    sends = [
        xcopy(0, x_ref, 0, lo, right), xcopy(1, x_ref, 1, hi, left),
        xcopy(2, x_ref, 0, hi, right), xcopy(3, x_ref, 1, lo, left),
    ]
    own_w = [wq_ref, wk_ref, wv_ref]
    wsend = [remote(own_w[n], wsib.at[n], wss.at[n], wrs.at[n], sib) for n in range(3)]
    for s in (sends[0], sends[1], *wsend, sends[2], sends[3]):
        s.start()

    pend = list(sends) + wsend
    arrive = []

    units = [(0, full), (nx - 1, lo), (1, hi), (nx - 1, hi), (1, lo), (2, lo), (2, hi)]

    def compute(u, src, rows):
        xv = src[rows, :]
        for w in range(2):
            if u == 0 and w == 1:
                for s in wsend:
                    s.wait_recv()
            for n in range(3):
                wref = own_w[n] if w == 0 else wsib.at[n]
                r = jnp.dot(xv, wref[...], preferred_element_type=F32).astype(BF16)
                kk = k if w == 0 else 1 - k
                for m in range(2):
                    stage[u, 2 * kk + m, n, rows, :] = r[:, m * HEAD:(m + 1) * HEAD]

    def block_of(u, d):
        dj, _ = units[u]
        return place((c + cp - d) % cp, (i + dj) % nx, k, cp)

    def send(u):
        rows = units[u][1]
        b = block_of(u, 0)
        for d in range(1, cp):
            cps = remote(stage.at[u, (c + d) % cp, :, rows], kvq.at[b, :, rows], ass.at[u, d], ars.at[u, d], peer[d])
            cps.start()
            pend.append(cps)
        lc = pltpu.make_async_copy(stage.at[u, c, :, rows], kvq.at[b, :, rows], ls.at[u])
        lc.start()
        locs.append(lc)
        relay(u, 0, stage.at[u, c, pl.ds(1, 2), rows])

    def relay(u, d, src):
        rows = units[u][1]
        b = block_of(u, d)
        cps = remote(src, kvq.at[b, pl.ds(1, 2), rows], rss.at[u, d], rrs.at[u, d], sib)
        cps.start()
        pend.append(cps)
        arrive.append((u, d))

    def pass_on(u):
        rows = units[u][1]
        for d in range(1, cp):
            b = block_of(u, d)
            remote(stage.at[u, 0, :, rows], kvq.at[b, :, rows], ass.at[u, d], ars.at[u, d], peer[d]).wait_recv()
            relay(u, d, kvq.at[b, pl.ds(1, 2), rows])

    locs = []
    compute(0, x_ref, full)
    send(0)
    sends[0].wait_recv()
    f = xcopy(4, xb.at[0], 2, lo, right)
    f.start()
    g = xcopy(5, xb.at[1], 2, hi, left)
    sends[1].wait_recv()
    g.start()
    pend += [f, g]
    compute(1, xb.at[0], lo)
    send(1)
    compute(2, xb.at[1], hi)
    send(2)
    pass_on(0)
    sends[2].wait_recv()
    compute(3, xb.at[0], hi)
    send(3)
    sends[3].wait_recv()
    compute(4, xb.at[1], lo)
    send(4)
    pass_on(1)
    pass_on(2)
    f.wait_recv()
    compute(5, xb.at[2], lo)
    send(5)
    g.wait_recv()
    compute(6, xb.at[2], hi)
    send(6)
    for u in range(3, 7):
        pass_on(u)
    for u, d in arrive:
        rows = units[u][1]
        b = block_of(u, d) + 1 - 2 * k
        remote(stage.at[u, 0, pl.ds(1, 2), rows], kvq.at[b, pl.ds(1, 2), rows], rss.at[u, d], rrs.at[u, d], sib).wait_recv()
    for lc in locs:
        lc.wait()
    for s in pend:
        s.wait_send()


def attn_kernel(cp, nx, kvq, wo_ref, x_ref, h_ref, vt, wof, ostage, obuf, sa, sb, acc, wss, wrs, oss, ors, ls):
    c = lax.axis_index('cp')
    t = lax.axis_index('tp')
    i, k = t // 2, t % 2
    T, H = x_ref.shape
    R = wo_ref.shape[0]
    nch = kvq.shape[0] // 2
    sib = {'cp': c, 'tp': i * 2 + 1 - k}
    ri, li, oi = (i + 1) % nx, (i + nx - 1) % nx, (i + 2) % nx
    right = {'cp': c, 'tp': ri * 2 + k}
    left = {'cp': c, 'tp': li * 2 + k}
    offs = [(di, dc) for di in range(nx) for dc in range(cp)]

    def dev(di, dc):
        return {'cp': (c + dc) % cp, 'tp': ((i + di) % nx) * 2 + k}

    barrier_with([sib] + [dev(di, dc) for di, dc in offs[1:]])
    half = R // 2
    lo, hi, full = pl.ds(0, half), pl.ds(half, half), pl.ds(0, R)
    def wcopy(n, src, chip, core, rows, to):
        return remote(src, wof.at[chip * 2 + core, rows], wss.at[n], wrs.at[n], to)

    w0 = wcopy(0, wo_ref.at[lo], i, k, lo, right)
    w1 = wcopy(1, wo_ref.at[hi], i, k, hi, left)
    w2 = wcopy(2, wo_ref.at[hi], i, k, hi, right)
    w3 = wcopy(3, wo_ref.at[lo], i, k, lo, left)
    w6 = wcopy(6, wo_ref, i, k, full, sib)
    for w in (w0, w1, w2, w3, w6):
        w.start()
    wl = pltpu.make_async_copy(wo_ref, wof.at[t], ls.at[0])
    wl.start()
    w4 = wcopy(4, wof.at[li * 2 + k, lo], li, k, lo, right)
    w5 = wcopy(5, wof.at[ri * 2 + k, hi], ri, k, hi, left)
    w7 = wcopy(7, wof.at[li * 2 + k], li, k, full, sib)
    w8 = wcopy(8, wof.at[ri * 2 + k], ri, k, full, sib)
    w9 = wcopy(9, wof.at[oi * 2 + k], oi, k, full, sib)

    @pl.loop(0, nch)
    def _(m):
        v = kvq[pl.ds(2 * m, 2), 2].reshape(2 * T, HEAD)
        vt[m] = v.astype(F32).T.astype(BF16)

    scale = HEAD ** -0.5 * math.log2(math.e)
    par = i % 2
    col_i = lax.broadcasted_iota(jnp.int32, (1, 2 * T), 1)
    qpos = col_i % T + k * T + 2 * T * jnp.where(col_i < T, par, 1 - par)
    row_i = lax.broadcasted_iota(jnp.int32, (2 * T, 2 * T), 0)

    def scores(q, m, buf):
        kb = kvq[pl.ds(2 * m, 2), 1].reshape(2 * T, HEAD)
        buf[...] = lax.dot_general(kb, q, (((1,), (1,)), ((), ())), preferred_element_type=F32)

    def absorb(buf, m, part, ml):
        mo, l = ml
        s = buf[...]
        if part is not None:
            s = jnp.where(row_i + 2 * T * part <= qpos, s, -jnp.inf)
        mn = jnp.maximum(mo, jnp.max(s, axis=0, keepdims=True))
        w = jnp.exp2((s - mn) * scale)
        a = jnp.exp2((mo - mn) * scale)
        l = l * a + jnp.sum(w, axis=0, keepdims=True)
        acc[...] = acc[...] * a + jnp.dot(vt[m], w.astype(BF16), preferred_element_type=F32)
        return mn, l

    def attend(n):
        cc = (c + n % cp) % cp
        high = (i // 2 + n // cp) % 2
        pb0 = place(cc, 2 * high + par, k, cp)
        pb1 = place(cc, 2 * high + 1 - par, k, cp)
        q = jnp.concatenate([kvq[pb0, 0], kvq[pb1, 0]], axis=0)
        p = pb0 // 4
        acc[...] = jnp.zeros_like(acc)
        scores(q, 0, sa)

        def body(j, ml):
            scores(q, 2 * j + 1, sb)
            ml = absorb(sa, 2 * j, None, ml)
            scores(q, 2 * j + 2, sa)
            return absorb(sb, 2 * j + 1, None, ml)

        ml = (jnp.full((1, 2 * T), -jnp.inf, F32), jnp.zeros((1, 2 * T), F32))
        ml = lax.fori_loop(0, p, body, ml)
        scores(q, 2 * p + 1, sb)
        ml = absorb(sa, 2 * p, 0, ml)
        _, l = absorb(sb, 2 * p + 1, 1, ml)
        o = (acc[...] / l).T.astype(BF16)
        ostage[n, 0] = o[:T]
        ostage[n, 1] = o[T:]

    col = pl.ds((c % 2) * HEAD, HEAD)
    npair = 2 * cp

    def owner(n, e, sign):
        chip = 2 * ((i // 2 + n // cp) % 2) + (par + e) % 2
        return {'cp': (c + sign * (n % cp) + cp) % cp, 'tp': chip * 2 + k}

    def osend(n, e):
        return remote(ostage.at[n, e], obuf.at[i * 2 + c // 2, :, col], oss.at[n, e], ors.at[n, e], owner(n, e, 1))

    def run(a, b):
        @pl.loop(a, b)
        def _(n):
            attend(n)
            osend(n, 0).start()
            osend(n, 1).start()

    run(1, 3)
    w0.wait_recv()
    w4.start()
    w1.wait_recv()
    w5.start()
    run(3, 5)
    w2.wait_recv()
    w7.start()
    w3.wait_recv()
    w8.start()
    run(5, npair)
    attend(0)
    osend(0, 1).start()
    lo_c = pltpu.make_async_copy(ostage.at[0, 0], obuf.at[i * 2 + c // 2, :, col], ls.at[1])
    lo_c.start()
    w4.wait_recv()
    w5.wait_recv()
    w9.start()
    wl.wait()
    for w in (w6, w7, w8, w9):
        w.wait_recv()
    lo_c.wait()
    osend(0, 1).wait_recv()

    @pl.loop(1, npair)
    def _(n):
        osend(n, 0).wait_recv()
        osend(n, 1).wait_recv()

    nt = wof.shape[0]
    cw = min(512, H)
    for j in range(H // cw):
        cs = slice(j * cw, (j + 1) * cw)
        a = jnp.dot(obuf[0], wof[0, :, cs], preferred_element_type=F32)
        for tt in range(1, nt):
            a += jnp.dot(obuf[tt], wof[tt, :, cs], preferred_element_type=F32)
        h_ref[:, cs] = (x_ref[:, cs].astype(F32) + a).astype(BF16)

    for w in (w0, w1, w2, w3, w4, w5, w6, w7, w8, w9):
        w.wait_send()

    osend(0, 1).wait_send()

    @pl.loop(1, npair)
    def _(n):
        osend(n, 0).wait_send()
        osend(n, 1).wait_send()


def moe_kernel(cp, tp, cap, h_ref, p_ref, g0_ref, g1_ref, gates_ref, wg_hbm, wu_hbm, wd_hbm, y_ref,
               sendb, recvb, zb, back, wg, wu, wd, acc0, acc1, wsem, dss, drs, bss, brs):
    c = lax.axis_index('cp')
    t = lax.axis_index('tp')
    ne = cp * tp
    T, H = h_ref.shape
    grp = 4
    ng = ne // grp
    wc = [pltpu.make_async_copy(a.at[0], b, wsem.at[n]) for n, (a, b) in enumerate(((wg_hbm, wg), (wu_hbm, wu), (wd_hbm, wd)))]
    for w in wc:
        w.start()

    nx = tp // 2
    i, k = t // 2, t % 2

    def offset(d):
        w = d // 2
        return w % cp, (w + w // cp) % nx, d % 2

    def fwd(d):
        dc, di, dk = offset(d)
        return {'cp': (c + dc) % cp, 'tp': ((i + di) % nx) * 2 + (k + dk) % 2}

    def bwd(d):
        dc, di, dk = offset(d)
        return {'cp': (c + cp - dc) % cp, 'tp': ((i + nx - di) % nx) * 2 + (k + dk) % 2}

    b = pltpu.get_barrier_semaphore()

    @pl.loop(1, ne)
    def _(d):
        pl.semaphore_signal(b, inc=1, device_id=fwd(d), device_id_type=MESH)

    def pack(g):
        rows = p_ref[pl.ds(g * grp * cap, grp * cap), :]
        r = jnp.dot(rows, h_ref[...], preferred_element_type=F32).astype(BF16)
        sendb[pl.ds(g * grp, grp)] = r.reshape(grp, cap, H)

    def disp(d):
        return remote(sendb.at[d], recvb.at[d], dss.at[d], drs.at[d], fwd(d))

    def ret(d):
        return remote(zb.at[d], back.at[d], bss.at[d], brs.at[d], bwd(d))

    pack(0)
    recvb[0] = sendb[0]
    pl.semaphore_wait(b, ne - 1)
    for d in range(1, grp):
        disp(d).start()

    @pl.loop(1, ng)
    def _(g):
        pack(g)
        for j in range(grp):
            disp(g * grp + j).start()

    for w in wc:
        w.wait()

    def ffn(g):
        rows = recvb[pl.ds(g * grp, grp)].reshape(grp * cap, H)
        gg = jnp.dot(rows, wg[...], preferred_element_type=F32)
        uu = jnp.dot(rows, wu[...], preferred_element_type=F32)
        act = (gg * jax.nn.sigmoid(gg) * uu).astype(BF16)
        z = jnp.dot(act, wd[...], preferred_element_type=F32).astype(BF16)
        zb[pl.ds(g * grp, grp)] = z.reshape(grp, cap, H)

    def combine(g):
        zz = back[pl.ds(g * grp, grp)].reshape(grp * cap, H)
        cols = pl.ds(pl.multiple_of(g * grp * cap, grp * cap), grp * cap)
        return (jnp.dot(g0_ref[:, cols], zz, preferred_element_type=F32),
                jnp.dot(g1_ref[:, cols], zz, preferred_element_type=F32))

    for d in range(1, grp):
        disp(d).wait_recv()
    ffn(0)
    back[0] = zb[0]
    for d in range(1, grp):
        ret(d).start()

    @pl.loop(1, ng)
    def _(g):
        for j in range(grp):
            disp(g * grp + j).wait_recv()
        ffn(g)
        for j in range(grp):
            ret(g * grp + j).start()

    for d in range(1, grp):
        ret(d).wait_recv()
    a, bb = combine(0)
    acc0[...] = a
    acc1[...] = bb

    @pl.loop(1, ng)
    def _(g):
        for j in range(grp):
            ret(g * grp + j).wait_recv()
        a, bb = combine(g)
        acc0[...] += a
        acc1[...] += bb

    y_ref[...] = (h_ref[...].astype(F32) + (gates_ref[:, 0:1] * acc0[...] + gates_ref[:, 1:2] * acc1[...])).astype(BF16)

    @pl.loop(1, ne)
    def _(d):
        disp(d).wait_send()
        ret(d).wait_send()


def params(cid):
    return pltpu.CompilerParams(collective_id=cid, has_side_effects=True, vmem_limit_bytes=60 * 1024 * 1024)


def attention(x, wq, wk, wv, wo, cp, tp):
    T, H = x.shape
    nx = tp // 2
    nb = cp * tp
    W = wq.shape[1]
    kvq = pl.pallas_call(
        functools.partial(qkv_kernel, cp, nx),
        out_shape=jax.ShapeDtypeStruct((nb, 3, T, HEAD), BF16),
        in_specs=[spec(VMEM)] * 4,
        out_specs=spec(VMEM),
        scratch_shapes=[
            VMEM((3, H, W), BF16), VMEM((3, T, H), BF16), VMEM((7, 4, 3, T, HEAD), BF16),
            DMA((3,)), DMA((3,)), DMA((6,)), DMA((6,)),
            DMA((7, cp)), DMA((7, cp)), DMA((7, cp)), DMA((7, cp)), DMA((7,)),
        ],
        compiler_params=params(0),
        name='qkv',
    )(x, wq, wk, wv)
    h = pl.pallas_call(
        functools.partial(attn_kernel, cp, nx),
        out_shape=jax.ShapeDtypeStruct((T, H), BF16),
        in_specs=[spec(VMEM)] * 3,
        out_specs=spec(VMEM),
        scratch_shapes=[
            VMEM((nb // 2, HEAD, 2 * T), BF16), VMEM((tp, wo.shape[0], H), BF16),
            VMEM((2 * cp, 2, T, HEAD), BF16), VMEM((tp, T, 2 * HEAD), BF16),
            VMEM((2 * T, 2 * T), F32), VMEM((2 * T, 2 * T), F32), VMEM((HEAD, 2 * T), F32),
            DMA((10,)), DMA((10,)), DMA((2 * cp, 2)), DMA((2 * cp, 2)), DMA((2,)),
        ],
        compiler_params=params(1),
        name='attn',
    )(kvq, wo, x)
    return h


def routing(idx, cp, tp, cap):
    ne = cp * tp
    T, kk = idx.shape
    c = lax.axis_index('cp')
    t = lax.axis_index('tp')
    nx = tp // 2
    dc = (idx // tp - c + cp) % cp
    di = (idx % tp // 2 - t // 2 + nx) % nx
    dk = (idx % 2 + t % 2) % 2
    rel = (((di - dc + nx) % nx) * cp + dc) * 2 + dk
    ea = rel.reshape(-1)
    onehot = (ea[:, None] == jnp.arange(ne)[None, :]).astype(jnp.int32)
    rank = jnp.cumsum(onehot, axis=0)
    slot = jnp.sum(onehot * rank, axis=1) - 1
    pos = (ea * cap + slot).reshape(T, kk)
    cols = jnp.arange(ne * cap, dtype=jnp.int32)
    g0 = pos[:, 0:1] == cols[None, :]
    g1 = pos[:, 1:2] == cols[None, :]
    p = (pos[:, 0][None, :] == cols[:, None]) | (pos[:, 1][None, :] == cols[:, None])
    return p.astype(BF16), g0.astype(BF16), g1.astype(BF16)


def experts(h, idx, gates, w1g, w1u, w2, cp, tp):
    T, H = h.shape
    F = w1g.shape[2]
    ne = cp * tp
    cap = 4 * T // ne
    p, g0, g1 = routing(idx, cp, tp, cap)
    return pl.pallas_call(
        functools.partial(moe_kernel, cp, tp, cap),
        out_shape=jax.ShapeDtypeStruct((T, H), BF16),
        in_specs=[spec(VMEM)] * 5 + [spec(pl.ANY)] * 3,
        out_specs=spec(VMEM),
        scratch_shapes=[VMEM((ne, cap, H), BF16)] * 4 + [
            VMEM((H, F), BF16), VMEM((H, F), BF16), VMEM((F, H), BF16), VMEM((T, H), F32), VMEM((T, H), F32),
            DMA((3,)), DMA((ne,)), DMA((ne,)), DMA((ne,)), DMA((ne,)),
        ],
        compiler_params=params(2),
        name='moe',
    )(h, p, g0, g1, gates, w1g, w1u, w2)


def solution(mesh):
    cp = mesh.shape['cp']
    tp = mesh.shape['tp']
    rows_spec = P(('dp', 'cp', 'tp'), None)
    exp_spec = P(('cp', 'tp'), None, None)

    def local(x, idx, gates, wq, wk, wv, wo, w1g, w1u, w2):
        h = attention(x, wq, wk, wv, wo, cp, tp)
        return experts(h, idx, gates, w1g, w1u, w2, cp, tp)

    return jax.shard_map(local, mesh=mesh, in_specs=(rows_spec, rows_spec, rows_spec, P(None, 'tp'), P(None, 'tp'), P(None, 'tp'), P('tp', None), exp_spec, exp_spec, exp_spec), out_specs=rows_spec, check_vma=False)
```

```python
import functools
import math

import jax
import jax.numpy as jnp
from jax import lax
from jax.experimental import pallas as pl
from jax.experimental.pallas import tpu as pltpu
from jax.sharding import PartitionSpec as P

HEAD = 128
MESH = pl.DeviceIdType.MESH
VMEM = pltpu.VMEM
DMA = pltpu.SemaphoreType.DMA
BF16 = jnp.bfloat16
F32 = jnp.float32


def spec(space):
    return pl.BlockSpec(memory_space=space)


def remote(src, dst, ssem, rsem, dev):
    return pltpu.make_async_remote_copy(src_ref=src, dst_ref=dst, send_sem=ssem, recv_sem=rsem, device_id=dev, device_id_type=MESH)


def barrier_with(devs):
    b = pltpu.get_barrier_semaphore()
    for d in devs:
        pl.semaphore_signal(b, inc=1, device_id=d, device_id_type=MESH)
    pl.semaphore_wait(b, len(devs))


def place(c, chip, core, cp):
    high = chip // 2
    seg = c * (1 - high) + (2 * cp - 1 - c) * high
    return seg * 4 + (chip % 2) * 2 + core


def slots(cp, nx, cap, c, i, k, idx_ref, pcol_ref, prow_ref):
    T = idx_ref.shape[0]
    tp = 2 * nx
    ne = cp * tp
    sh = tp.bit_length() - 1
    e = idx_ref[...]
    dc = ((e >> sh) - c) & (cp - 1)
    di = (((e & (tp - 1)) >> 1) - i) & (nx - 1)
    dk = (e - k) & 1
    rel = ((((di - dc) & (nx - 1)) * cp + dc) * 2 + dk)
    lanes = lax.broadcasted_iota(jnp.int32, (T, ne), 1)
    o0 = (rel[:, 0:1] == lanes).astype(F32)
    o1 = (rel[:, 1:2] == lanes).astype(F32)
    low = lax.broadcasted_iota(jnp.int32, (T, T), 0) > lax.broadcasted_iota(jnp.int32, (T, T), 1)
    prev = jnp.dot(low.astype(F32).astype(BF16), (o0 + o1).astype(BF16), preferred_element_type=F32)
    p0 = rel[:, 0:1] * cap + jnp.sum(prev * o0, axis=1, keepdims=True).astype(jnp.int32)
    p1 = rel[:, 1:2] * cap + jnp.sum(prev * o1, axis=1, keepdims=True).astype(jnp.int32)
    pcol_ref[:, 0:1] = p0
    pcol_ref[:, 1:2] = p1
    wide = (T, HEAD)
    prow_ref[0:1, :] = jnp.broadcast_to(p0.astype(F32), wide).T[0:1, :].astype(jnp.int32)
    prow_ref[1:2, :] = jnp.broadcast_to(p1.astype(F32), wide).T[0:1, :].astype(jnp.int32)


def attn_kernel(cp, nx, cap, x_ref, wq_ref, wk_ref, wv_ref, wo_ref, idx_ref, h_ref, pcol_ref, prow_ref,
                kvq, wsib, xb, stage, vt, wof, ostage, obuf, sa, sb, acc,
                wss, wrs, xss, xrs, ass, ars, rss, rrs, qls, wos, wor, oss, ors, ls):
    c = lax.axis_index('cp')
    t = lax.axis_index('tp')
    i, k = t // 2, t % 2
    T, H = x_ref.shape
    half = T // 2
    sib = {'cp': c, 'tp': i * 2 + 1 - k}
    right = {'cp': c, 'tp': ((i + 1) % nx) * 2 + k}
    left = {'cp': c, 'tp': ((i + nx - 1) % nx) * 2 + k}
    peer = [{'cp': (c + d) % cp, 'tp': t} for d in range(cp)]
    same = [{'cp': (c + dc) % cp, 'tp': ((i + di) % nx) * 2 + k} for di in range(nx) for dc in range(cp)]
    barrier_with([sib] + same[1:])
    lo, hi = pl.ds(0, half), pl.ds(half, half)
    full = pl.ds(0, T)

    R = wo_ref.shape[0]
    hr = R // 2
    rlo, rhi, rfull = pl.ds(0, hr), pl.ds(hr, hr), pl.ds(0, R)
    ri, li, oi = (i + 1) % nx, (i + nx - 1) % nx, (i + 2) % nx
    def wcopy(n, src, chip, core, rows, to):
        return remote(src, wof.at[chip * 2 + core, rows], wos.at[n], wor.at[n], to)

    w0 = wcopy(0, wo_ref.at[rlo], i, k, rlo, right)
    w1 = wcopy(1, wo_ref.at[rhi], i, k, rhi, left)
    w2 = wcopy(2, wo_ref.at[rhi], i, k, rhi, right)
    w3 = wcopy(3, wo_ref.at[rlo], i, k, rlo, left)
    w6 = wcopy(6, wo_ref, i, k, rfull, sib)
    wl = pltpu.make_async_copy(wo_ref, wof.at[t], ls.at[0])
    w4 = wcopy(4, wof.at[li * 2 + k, rlo], li, k, rlo, right)
    w5 = wcopy(5, wof.at[ri * 2 + k, rhi], ri, k, rhi, left)
    w7 = wcopy(7, wof.at[li * 2 + k], li, k, rfull, sib)
    w8 = wcopy(8, wof.at[ri * 2 + k], ri, k, rfull, sib)
    w9 = wcopy(9, wof.at[oi * 2 + k], oi, k, rfull, sib)


    def xcopy(n, src, slot, rows, dev):
        return remote(src.at[rows], xb.at[slot, rows], xss.at[n], xrs.at[n], dev)

    sends = [
        xcopy(0, x_ref, 0, lo, right), xcopy(1, x_ref, 1, hi, left),
        xcopy(2, x_ref, 0, hi, right), xcopy(3, x_ref, 1, lo, left),
    ]
    own_w = [wq_ref, wk_ref, wv_ref]
    wsend = [remote(own_w[n], wsib.at[n], wss.at[n], wrs.at[n], sib) for n in range(3)]
    for s in (sends[0], sends[1], *wsend, sends[2], sends[3]):
        s.start()

    pend = list(sends) + wsend
    arrive = []

    units = [(0, full), (nx - 1, lo), (1, hi), (nx - 1, hi), (1, lo), (2, lo), (2, hi)]

    def compute(u, src, rows):
        xv = src[rows, :]
        for w in range(2):
            if u == 0 and w == 1:
                for s in wsend:
                    s.wait_recv()
            for n in range(3):
                wref = own_w[n] if w == 0 else wsib.at[n]
                r = jnp.dot(xv, wref[...], preferred_element_type=F32).astype(BF16)
                kk = k if w == 0 else 1 - k
                for m in range(2):
                    stage[u, 2 * kk + m, n, rows, :] = r[:, m * HEAD:(m + 1) * HEAD]

    def block_of(u, d):
        dj, _ = units[u]
        return place((c + cp - d) % cp, (i + dj) % nx, k, cp)

    def send(u):
        rows = units[u][1]
        b = block_of(u, 0)
        for d in range(1, cp):
            cps = remote(stage.at[u, (c + d) % cp, :, rows], kvq.at[b, :, rows], ass.at[u, d], ars.at[u, d], peer[d])
            cps.start()
            pend.append(cps)
        lc = pltpu.make_async_copy(stage.at[u, c, :, rows], kvq.at[b, :, rows], qls.at[u])
        lc.start()
        locs.append(lc)
        relay(u, 0, stage.at[u, c, pl.ds(1, 2), rows])

    def relay(u, d, src):
        rows = units[u][1]
        b = block_of(u, d)
        cps = remote(src, kvq.at[b, pl.ds(1, 2), rows], rss.at[u, d], rrs.at[u, d], sib)
        cps.start()
        pend.append(cps)
        arrive.append((u, d))

    def pass_on(u):
        rows = units[u][1]
        for d in range(1, cp):
            b = block_of(u, d)
            remote(stage.at[u, 0, :, rows], kvq.at[b, :, rows], ass.at[u, d], ars.at[u, d], peer[d]).wait_recv()
            relay(u, d, kvq.at[b, pl.ds(1, 2), rows])

    locs = []
    compute(0, x_ref, full)
    send(0)
    slots(cp, nx, cap, c, i, k, idx_ref, pcol_ref, prow_ref)
    sends[0].wait_recv()
    f = xcopy(4, xb.at[0], 2, lo, right)
    f.start()
    g = xcopy(5, xb.at[1], 2, hi, left)
    sends[1].wait_recv()
    g.start()
    pend += [f, g]
    for w in (w0, w1, w2, w3, w6):
        w.start()
    wl.start()
    compute(1, xb.at[0], lo)
    send(1)
    compute(2, xb.at[1], hi)
    send(2)
    pass_on(0)
    sends[2].wait_recv()
    compute(3, xb.at[0], hi)
    send(3)
    sends[3].wait_recv()
    compute(4, xb.at[1], lo)
    send(4)
    pass_on(1)
    pass_on(2)
    f.wait_recv()
    compute(5, xb.at[2], lo)
    send(5)
    g.wait_recv()
    compute(6, xb.at[2], hi)
    send(6)
    for u in range(3, 7):
        pass_on(u)
    for u, d in arrive:
        rows = units[u][1]
        b = block_of(u, d) + 1 - 2 * k
        remote(stage.at[u, 0, pl.ds(1, 2), rows], kvq.at[b, pl.ds(1, 2), rows], rss.at[u, d], rrs.at[u, d], sib).wait_recv()
    for lc in locs:
        lc.wait()

    w0.wait_recv()
    w4.start()
    w1.wait_recv()
    w5.start()
    nch = kvq.shape[0] // 2

    @pl.loop(0, nch)
    def _(m):
        v = kvq[pl.ds(2 * m, 2), 2].reshape(2 * T, HEAD)
        vt[m] = v.astype(F32).T.astype(BF16)

    scale = HEAD ** -0.5 * math.log2(math.e)
    par = i % 2
    col_i = lax.broadcasted_iota(jnp.int32, (1, 2 * T), 1)
    qpos = col_i % T + k * T + 2 * T * jnp.where(col_i < T, par, 1 - par)
    row_i = lax.broadcasted_iota(jnp.int32, (2 * T, 2 * T), 0)

    def scores(q, m, buf):
        kb = kvq[pl.ds(2 * m, 2), 1].reshape(2 * T, HEAD)
        buf[...] = lax.dot_general(kb, q, (((1,), (1,)), ((), ())), preferred_element_type=F32)

    def absorb(buf, m, part, ml):
        mo, l = ml
        s = buf[...]
        if part is not None:
            s = jnp.where(row_i + 2 * T * part <= qpos, s, -jnp.inf)
        mn = jnp.maximum(mo, jnp.max(s, axis=0, keepdims=True))
        w = jnp.exp2((s - mn) * scale)
        a = jnp.exp2((mo - mn) * scale)
        l = l * a + jnp.sum(w, axis=0, keepdims=True)
        acc[...] = acc[...] * a + jnp.dot(vt[m], w.astype(BF16), preferred_element_type=F32)
        return mn, l

    def attend(n):
        cc = (c + n % cp) % cp
        high = (i // 2 + n // cp) % 2
        pb0 = place(cc, 2 * high + par, k, cp)
        pb1 = place(cc, 2 * high + 1 - par, k, cp)
        q = jnp.concatenate([kvq[pb0, 0], kvq[pb1, 0]], axis=0)
        p = pb0 // 4
        acc[...] = jnp.zeros_like(acc)
        scores(q, 0, sa)

        def body(j, ml):
            scores(q, 2 * j + 1, sb)
            ml = absorb(sa, 2 * j, None, ml)
            scores(q, 2 * j + 2, sa)
            return absorb(sb, 2 * j + 1, None, ml)

        ml = (jnp.full((1, 2 * T), -jnp.inf, F32), jnp.zeros((1, 2 * T), F32))
        ml = lax.fori_loop(0, p, body, ml)
        scores(q, 2 * p + 1, sb)
        ml = absorb(sa, 2 * p, 0, ml)
        _, l = absorb(sb, 2 * p + 1, 1, ml)
        o = (acc[...] / l).T.astype(BF16)
        ostage[n, 0] = o[:T]
        ostage[n, 1] = o[T:]

    col = pl.ds((c % 2) * HEAD, HEAD)
    npair = 2 * cp

    def owner(n, e, sign):
        chip = 2 * ((i // 2 + n // cp) % 2) + (par + e) % 2
        return {'cp': (c + sign * (n % cp) + cp) % cp, 'tp': chip * 2 + k}

    def osend(n, e):
        return remote(ostage.at[n, e], obuf.at[i * 2 + c // 2, :, col], oss.at[n, e], ors.at[n, e], owner(n, e, 1))

    def run(a, b):
        @pl.loop(a, b)
        def _(n):
            attend(n)
            osend(n, 0).start()
            osend(n, 1).start()

    run(1, 4)
    w2.wait_recv()
    w7.start()
    w3.wait_recv()
    w8.start()
    run(4, npair)
    attend(0)
    osend(0, 1).start()
    lo_c = pltpu.make_async_copy(ostage.at[0, 0], obuf.at[i * 2 + c // 2, :, col], ls.at[1])
    lo_c.start()
    w4.wait_recv()
    w5.wait_recv()
    w9.start()
    wl.wait()
    for w in (w6, w7, w8, w9):
        w.wait_recv()
    lo_c.wait()
    osend(0, 1).wait_recv()

    @pl.loop(1, npair)
    def _(n):
        osend(n, 0).wait_recv()
        osend(n, 1).wait_recv()

    nt = wof.shape[0]
    cw = min(512, H)
    for j in range(H // cw):
        cs = slice(j * cw, (j + 1) * cw)
        a = jnp.dot(obuf[0], wof[0, :, cs], preferred_element_type=F32)
        for tt in range(1, nt):
            a += jnp.dot(obuf[tt], wof[tt, :, cs], preferred_element_type=F32)
        h_ref[:, cs] = (x_ref[:, cs].astype(F32) + a).astype(BF16)

    for w in (w0, w1, w2, w3, w4, w5, w6, w7, w8, w9):
        w.wait_send()

    osend(0, 1).wait_send()

    @pl.loop(1, npair)
    def _(n):
        osend(n, 0).wait_send()
        osend(n, 1).wait_send()
    for s in pend:
        s.wait_send()


def moe_kernel(cp, tp, cap, h_ref, pcol_ref, prow_ref, gates_ref, wg_hbm, wu_hbm, wd_hbm, y_ref,
               sendb, recvb, zb, back, wg, wu, wd, acc, wsem, dss, drs, bss, brs):
    c = lax.axis_index('cp')
    t = lax.axis_index('tp')
    ne = cp * tp
    T, H = h_ref.shape
    grp = 4
    ng = ne // grp
    wc = [pltpu.make_async_copy(a.at[0], b, wsem.at[n]) for n, (a, b) in enumerate(((wg_hbm, wg), (wu_hbm, wu), (wd_hbm, wd)))]
    for w in wc:
        w.start()

    nx = tp // 2
    i, k = t // 2, t % 2

    def offset(d):
        w = d // 2
        return w % cp, (w + w // cp) % nx, d % 2

    def fwd(d):
        dc, di, dk = offset(d)
        return {'cp': (c + dc) % cp, 'tp': ((i + di) % nx) * 2 + (k + dk) % 2}

    def bwd(d):
        dc, di, dk = offset(d)
        return {'cp': (c + cp - dc) % cp, 'tp': ((i + nx - di) % nx) * 2 + (k + dk) % 2}

    b = pltpu.get_barrier_semaphore()

    @pl.loop(1, ne)
    def _(d):
        pl.semaphore_signal(b, inc=1, device_id=fwd(d), device_id_type=MESH)

    def pack(g):
        s = lax.broadcasted_iota(jnp.int32, (grp * cap, T), 0) + g * (grp * cap)
        pick = jnp.where((s == prow_ref[0:1, :]) | (s == prow_ref[1:2, :]), 1.0, 0.0).astype(BF16)
        r = jnp.dot(pick, h_ref[...], preferred_element_type=F32).astype(BF16)
        sendb[pl.ds(g * grp, grp)] = r.reshape(grp, cap, H)

    def disp(d):
        return remote(sendb.at[d], recvb.at[d], dss.at[d], drs.at[d], fwd(d))

    def ret(d):
        return remote(zb.at[d], back.at[d], bss.at[d], brs.at[d], bwd(d))

    pack(0)
    recvb[0] = sendb[0]
    pl.semaphore_wait(b, ne - 1)
    for d in range(1, grp):
        disp(d).start()

    @pl.loop(1, ng)
    def _(g):
        pack(g)
        for j in range(grp):
            disp(g * grp + j).start()

    for w in wc:
        w.wait()

    def ffn(g):
        rows = recvb[pl.ds(g * grp, grp)].reshape(grp * cap, H)
        gg = jnp.dot(rows, wg[...], preferred_element_type=F32)
        uu = jnp.dot(rows, wu[...], preferred_element_type=F32)
        act = (gg * jax.nn.sigmoid(gg) * uu).astype(BF16)
        z = jnp.dot(act, wd[...], preferred_element_type=F32).astype(BF16)
        zb[pl.ds(g * grp, grp)] = z.reshape(grp, cap, H)

    def combine(g):
        zz = back[pl.ds(g * grp, grp)].reshape(grp * cap, H)
        s = lax.broadcasted_iota(jnp.int32, (T, grp * cap), 1) + g * (grp * cap)
        g0 = jnp.where(s == pcol_ref[:, 0:1], 1.0, 0.0).astype(BF16)
        g1 = jnp.where(s == pcol_ref[:, 1:2], 1.0, 0.0).astype(BF16)
        return (gates_ref[:, 0:1] * jnp.dot(g0, zz, preferred_element_type=F32)
                + gates_ref[:, 1:2] * jnp.dot(g1, zz, preferred_element_type=F32))

    for d in range(1, grp):
        disp(d).wait_recv()
    ffn(0)
    back[0] = zb[0]
    for d in range(1, grp):
        ret(d).start()

    @pl.loop(1, ng)
    def _(g):
        for j in range(grp):
            disp(g * grp + j).wait_recv()
        ffn(g)
        for j in range(grp):
            ret(g * grp + j).start()

    for d in range(1, grp):
        ret(d).wait_recv()
    acc[...] = h_ref[...].astype(F32) + combine(0)

    @pl.loop(1, ng)
    def _(g):
        for j in range(grp):
            ret(g * grp + j).wait_recv()
        acc[...] += combine(g)

    y_ref[...] = acc[...].astype(BF16)

    @pl.loop(1, ne)
    def _(d):
        disp(d).wait_send()
        ret(d).wait_send()


def params(cid):
    return pltpu.CompilerParams(collective_id=cid, has_side_effects=True, vmem_limit_bytes=60 * 1024 * 1024)


def attention(x, idx, wq, wk, wv, wo, cp, tp, cap):
    T, H = x.shape
    nx = tp // 2
    nb = cp * tp
    W = wq.shape[1]
    return pl.pallas_call(
        functools.partial(attn_kernel, cp, nx, cap),
        out_shape=[
            jax.ShapeDtypeStruct((T, H), BF16), jax.ShapeDtypeStruct(idx.shape, jnp.int32), jax.ShapeDtypeStruct((2, T), jnp.int32),
        ],
        in_specs=[spec(VMEM)] * 6,
        out_specs=[spec(VMEM)] * 3,
        scratch_shapes=[
            VMEM((nb, 3, T, HEAD), BF16), VMEM((3, H, W), BF16), VMEM((3, T, H), BF16), VMEM((7, 4, 3, T, HEAD), BF16),
            VMEM((nb // 2, HEAD, 2 * T), BF16), VMEM((tp, wo.shape[0], H), BF16),
            VMEM((2 * cp, 2, T, HEAD), BF16), VMEM((tp, T, 2 * HEAD), BF16),
            VMEM((2 * T, 2 * T), F32), VMEM((2 * T, 2 * T), F32), VMEM((HEAD, 2 * T), F32),
            DMA((3,)), DMA((3,)), DMA((6,)), DMA((6,)),
            DMA((7, cp)), DMA((7, cp)), DMA((7, cp)), DMA((7, cp)), DMA((7,)),
            DMA((10,)), DMA((10,)), DMA((2 * cp, 2)), DMA((2 * cp, 2)), DMA((2,)),
        ],
        compiler_params=params(0),
        name='attn',
    )(x, wq, wk, wv, wo, idx)


def experts(h, pcol, prow, gates, w1g, w1u, w2, cp, tp, cap):
    T, H = h.shape
    F = w1g.shape[2]
    ne = cp * tp
    return pl.pallas_call(
        functools.partial(moe_kernel, cp, tp, cap),
        out_shape=jax.ShapeDtypeStruct((T, H), BF16),
        in_specs=[spec(VMEM)] * 4 + [spec(pl.ANY)] * 3,
        out_specs=spec(VMEM),
        scratch_shapes=[VMEM((ne, cap, H), BF16)] * 4 + [
            VMEM((H, F), BF16), VMEM((H, F), BF16), VMEM((F, H), BF16), VMEM((T, H), F32),
            DMA((3,)), DMA((ne,)), DMA((ne,)), DMA((ne,)), DMA((ne,)),
        ],
        compiler_params=params(1),
        name='moe',
    )(h, pcol, prow, gates, w1g, w1u, w2)


def solution(mesh):
    cp = mesh.shape['cp']
    tp = mesh.shape['tp']
    rows_spec = P(('dp', 'cp', 'tp'), None)
    exp_spec = P(('cp', 'tp'), None, None)

    def local(x, idx, gates, wq, wk, wv, wo, w1g, w1u, w2):
        cap = 4 * x.shape[0] // (cp * tp)
        h, pcol, prow = attention(x, idx, wq, wk, wv, wo, cp, tp, cap)
        return experts(h, pcol, prow, gates, w1g, w1u, w2, cp, tp, cap)

    return jax.shard_map(local, mesh=mesh, in_specs=(rows_spec, rows_spec, rows_spec, P(None, 'tp'), P(None, 'tp'), P(None, 'tp'), P('tp', None), exp_spec, exp_spec, exp_spec), out_specs=rows_spec, check_vma=False)
```

```python
import functools
import math

import jax
import jax.numpy as jnp
from jax import lax
from jax.experimental import pallas as pl
from jax.experimental.pallas import tpu as pltpu
from jax.sharding import PartitionSpec as P

HEAD = 128
MESH = pl.DeviceIdType.MESH
VMEM = pltpu.VMEM
DMA = pltpu.SemaphoreType.DMA
BF16 = jnp.bfloat16
F32 = jnp.float32


def spec(space):
    return pl.BlockSpec(memory_space=space)


def remote(src, dst, ssem, rsem, dev):
    return pltpu.make_async_remote_copy(src_ref=src, dst_ref=dst, send_sem=ssem, recv_sem=rsem, device_id=dev, device_id_type=MESH)


def barrier_with(devs):
    b = pltpu.get_barrier_semaphore()
    for d in devs:
        pl.semaphore_signal(b, inc=1, device_id=d, device_id_type=MESH)
    pl.semaphore_wait(b, len(devs))


def place(c, chip, core, cp):
    high = chip // 2
    seg = c * (1 - high) + (2 * cp - 1 - c) * high
    return seg * 4 + (chip % 2) * 2 + core


def slots(cp, nx, cap, c, i, k, idx_ref, prow_ref):
    T = idx_ref.shape[1]
    tp = 2 * nx
    ne = cp * tp
    sh = tp.bit_length() - 1
    e = idx_ref[...]
    dc = ((e >> sh) - c) & (cp - 1)
    di = (((e & (tp - 1)) >> 1) - i) & (nx - 1)
    dk = (e - k) & 1
    rel = ((((di - dc) & (nx - 1)) * cp + dc) * 2 + dk)
    experts_i = lax.broadcasted_iota(jnp.int32, (ne, T), 0)
    o0 = (rel[0:1, :] == experts_i).astype(F32)
    o1 = (rel[1:2, :] == experts_i).astype(F32)
    low = lax.broadcasted_iota(jnp.int32, (T, T), 0) < lax.broadcasted_iota(jnp.int32, (T, T), 1)
    prev = jnp.dot((o0 + o1).astype(BF16), low.astype(F32).astype(BF16), preferred_element_type=F32)
    p0 = rel[0:1, :] * cap + jnp.sum(prev * o0, axis=0, keepdims=True).astype(jnp.int32)
    p1 = rel[1:2, :] * cap + jnp.sum(prev * o1, axis=0, keepdims=True).astype(jnp.int32)
    prow_ref[0:1, :] = p0
    prow_ref[1:2, :] = p1


def attn_kernel(cp, nx, cap, x_ref, wq_ref, wk_ref, wv_ref, wo_ref, idx_ref, h_ref, prow_ref,
                kvq, wsib, xb, stage, vt, wof, ostage, obuf, sa, sb, acc,
                wss, wrs, xss, xrs, ass, ars, rss, rrs, qls, wos, wor, oss, ors, ls):
    c = lax.axis_index('cp')
    t = lax.axis_index('tp')
    i, k = t // 2, t % 2
    T, H = x_ref.shape
    half = T // 2
    sib = {'cp': c, 'tp': i * 2 + 1 - k}
    right = {'cp': c, 'tp': ((i + 1) % nx) * 2 + k}
    left = {'cp': c, 'tp': ((i + nx - 1) % nx) * 2 + k}
    peer = [{'cp': (c + d) % cp, 'tp': t} for d in range(cp)]
    same = [{'cp': (c + dc) % cp, 'tp': ((i + di) % nx) * 2 + k} for di in range(nx) for dc in range(cp)]
    barrier_with([sib] + same[1:])
    lo, hi = pl.ds(0, half), pl.ds(half, half)
    full = pl.ds(0, T)

    R = wo_ref.shape[0]
    hr = R // 2
    rlo, rhi, rfull = pl.ds(0, hr), pl.ds(hr, hr), pl.ds(0, R)
    ri, li, oi = (i + 1) % nx, (i + nx - 1) % nx, (i + 2) % nx
    def wcopy(n, src, chip, core, rows, to):
        return remote(src, wof.at[chip * 2 + core, rows], wos.at[n], wor.at[n], to)

    w0 = wcopy(0, wo_ref.at[rlo], i, k, rlo, right)
    w1 = wcopy(1, wo_ref.at[rhi], i, k, rhi, left)
    w2 = wcopy(2, wo_ref.at[rhi], i, k, rhi, right)
    w3 = wcopy(3, wo_ref.at[rlo], i, k, rlo, left)
    w6 = wcopy(6, wo_ref, i, k, rfull, sib)
    wl = pltpu.make_async_copy(wo_ref, wof.at[t], ls.at[0])
    w4 = wcopy(4, wof.at[li * 2 + k, rlo], li, k, rlo, right)
    w5 = wcopy(5, wof.at[ri * 2 + k, rhi], ri, k, rhi, left)
    w7 = wcopy(7, wof.at[li * 2 + k], li, k, rfull, sib)
    w8 = wcopy(8, wof.at[ri * 2 + k], ri, k, rfull, sib)
    w9 = wcopy(9, wof.at[oi * 2 + k], oi, k, rfull, sib)


    def xcopy(n, src, slot, rows, dev):
        return remote(src.at[rows], xb.at[slot, rows], xss.at[n], xrs.at[n], dev)

    sends = [
        xcopy(0, x_ref, 0, lo, right), xcopy(1, x_ref, 1, hi, left),
        xcopy(2, x_ref, 0, hi, right), xcopy(3, x_ref, 1, lo, left),
    ]
    own_w = [wq_ref, wk_ref, wv_ref]
    wsend = [remote(own_w[n], wsib.at[n], wss.at[n], wrs.at[n], sib) for n in range(3)]
    for s in (sends[0], sends[1], *wsend, sends[2], sends[3]):
        s.start()

    pend = list(sends) + wsend
    arrive = []

    units = [(0, full), (nx - 1, lo), (1, hi), (nx - 1, hi), (1, lo), (2, lo), (2, hi)]

    def compute(u, src, rows):
        xv = src[rows, :]
        for w in range(2):
            if u == 0 and w == 1:
                for s in wsend:
                    s.wait_recv()
            for n in range(3):
                wref = own_w[n] if w == 0 else wsib.at[n]
                r = jnp.dot(xv, wref[...], preferred_element_type=F32).astype(BF16)
                kk = k if w == 0 else 1 - k
                for m in range(2):
                    stage[u, 2 * kk + m, n, rows, :] = r[:, m * HEAD:(m + 1) * HEAD]

    def block_of(u, d):
        dj, _ = units[u]
        return place((c + cp - d) % cp, (i + dj) % nx, k, cp)

    def send(u):
        rows = units[u][1]
        b = block_of(u, 0)
        for d in range(1, cp):
            cps = remote(stage.at[u, (c + d) % cp, :, rows], kvq.at[b, :, rows], ass.at[u, d], ars.at[u, d], peer[d])
            cps.start()
            pend.append(cps)
        lc = pltpu.make_async_copy(stage.at[u, c, :, rows], kvq.at[b, :, rows], qls.at[u])
        lc.start()
        locs.append(lc)
        relay(u, 0, stage.at[u, c, pl.ds(1, 2), rows])

    def relay(u, d, src):
        rows = units[u][1]
        b = block_of(u, d)
        cps = remote(src, kvq.at[b, pl.ds(1, 2), rows], rss.at[u, d], rrs.at[u, d], sib)
        cps.start()
        pend.append(cps)
        arrive.append((u, d))

    def pass_on(u):
        rows = units[u][1]
        for d in range(1, cp):
            b = block_of(u, d)
            remote(stage.at[u, 0, :, rows], kvq.at[b, :, rows], ass.at[u, d], ars.at[u, d], peer[d]).wait_recv()
            relay(u, d, kvq.at[b, pl.ds(1, 2), rows])

    locs = []
    compute(0, x_ref, full)
    send(0)
    slots(cp, nx, cap, c, i, k, idx_ref, prow_ref)
    sends[0].wait_recv()
    f = xcopy(4, xb.at[0], 2, lo, right)
    f.start()
    g = xcopy(5, xb.at[1], 2, hi, left)
    sends[1].wait_recv()
    g.start()
    pend += [f, g]
    for w in (w0, w1, w2, w3, w6):
        w.start()
    wl.start()
    compute(1, xb.at[0], lo)
    send(1)
    compute(2, xb.at[1], hi)
    send(2)
    pass_on(0)
    sends[2].wait_recv()
    compute(3, xb.at[0], hi)
    send(3)
    sends[3].wait_recv()
    compute(4, xb.at[1], lo)
    send(4)
    pass_on(1)
    pass_on(2)
    f.wait_recv()
    compute(5, xb.at[2], lo)
    send(5)
    g.wait_recv()
    compute(6, xb.at[2], hi)
    send(6)
    for u in range(3, 7):
        pass_on(u)
    for u, d in arrive:
        rows = units[u][1]
        b = block_of(u, d) + 1 - 2 * k
        remote(stage.at[u, 0, pl.ds(1, 2), rows], kvq.at[b, pl.ds(1, 2), rows], rss.at[u, d], rrs.at[u, d], sib).wait_recv()
    for lc in locs:
        lc.wait()

    w0.wait_recv()
    w4.start()
    w1.wait_recv()
    w5.start()
    nch = kvq.shape[0] // 2

    @pl.loop(0, nch)
    def _(m):
        v = kvq[pl.ds(2 * m, 2), 2].reshape(2 * T, HEAD)
        vt[m] = v.astype(F32).T.astype(BF16)

    scale = HEAD ** -0.5 * math.log2(math.e)
    par = i % 2
    col_i = lax.broadcasted_iota(jnp.int32, (1, 2 * T), 1)
    qpos = col_i % T + k * T + 2 * T * jnp.where(col_i < T, par, 1 - par)
    row_i = lax.broadcasted_iota(jnp.int32, (2 * T, 2 * T), 0)

    def scores(q, m, part, buf):
        kb = kvq[pl.ds(2 * m, 2), 1].reshape(2 * T, HEAD)
        s = lax.dot_general(kb, q, (((1,), (1,)), ((), ())), preferred_element_type=F32)
        if part is not None:
            s = jnp.where(row_i + 2 * T * part <= qpos, s, -jnp.inf)
        buf[...] = s
        return jnp.max(s, axis=0, keepdims=True)

    def absorb(buf, m, top, ml):
        mo, l = ml
        mn = jnp.maximum(mo, top)
        w = jnp.exp2((buf[...] - mn) * scale)
        a = jnp.exp2((mo - mn) * scale)
        l = l * a + jnp.sum(w, axis=0, keepdims=True)
        acc[...] = acc[...] * a + jnp.dot(vt[m], w.astype(BF16), preferred_element_type=F32)
        return mn, l

    def attend(n):
        cc = (c + n % cp) % cp
        high = (i // 2 + n // cp) % 2
        pb0 = place(cc, 2 * high + par, k, cp)
        pb1 = place(cc, 2 * high + 1 - par, k, cp)
        q = jnp.concatenate([kvq[pb0, 0], kvq[pb1, 0]], axis=0)
        p = pb0 // 4
        acc[...] = jnp.zeros_like(acc)
        last = p * 2

        def body(j, carry):
            ml, ta = carry
            tb = scores(q, 2 * j + 1, None, sb)
            ml = absorb(sa, 2 * j, ta, ml)
            ta = scores(q, 2 * j + 2, None, sa)
            return absorb(sb, 2 * j + 1, tb, ml), ta

        ml = (jnp.full((1, 2 * T), -jnp.inf, F32), jnp.zeros((1, 2 * T), F32))
        ta = scores(q, 0, None, sa)
        ml, ta = lax.fori_loop(0, p, body, (ml, ta))
        s = jnp.where(row_i <= qpos, sa[...], -jnp.inf)
        sa[...] = s
        ta = jnp.max(s, axis=0, keepdims=True)
        tb = scores(q, last + 1, 1, sb)
        ml = absorb(sa, last, ta, ml)
        _, l = absorb(sb, last + 1, tb, ml)
        o = (acc[...] / l).T.astype(BF16)
        ostage[n, 0] = o[:T]
        ostage[n, 1] = o[T:]

    col = pl.ds((c % 2) * HEAD, HEAD)
    npair = 2 * cp

    def owner(n, e, sign):
        chip = 2 * ((i // 2 + n // cp) % 2) + (par + e) % 2
        return {'cp': (c + sign * (n % cp) + cp) % cp, 'tp': chip * 2 + k}

    def osend(n, e):
        return remote(ostage.at[n, e], obuf.at[i * 2 + c // 2, :, col], oss.at[n, e], ors.at[n, e], owner(n, e, 1))

    def run(a, b):
        @pl.loop(a, b)
        def _(n):
            attend(n)
            osend(n, 0).start()
            osend(n, 1).start()

    run(1, 4)
    w2.wait_recv()
    w7.start()
    w3.wait_recv()
    w8.start()
    run(4, npair)
    attend(0)
    osend(0, 1).start()
    lo_c = pltpu.make_async_copy(ostage.at[0, 0], obuf.at[i * 2 + c // 2, :, col], ls.at[1])
    lo_c.start()
    w4.wait_recv()
    w5.wait_recv()
    w9.start()
    wl.wait()
    for w in (w6, w7, w8, w9):
        w.wait_recv()
    lo_c.wait()
    osend(0, 1).wait_recv()

    @pl.loop(1, npair)
    def _(n):
        osend(n, 0).wait_recv()
        osend(n, 1).wait_recv()

    nt = wof.shape[0]
    cw = min(512, H)
    for j in range(H // cw):
        cs = slice(j * cw, (j + 1) * cw)
        a = jnp.dot(obuf[0], wof[0, :, cs], preferred_element_type=F32)
        for tt in range(1, nt):
            a += jnp.dot(obuf[tt], wof[tt, :, cs], preferred_element_type=F32)
        h_ref[:, cs] = (x_ref[:, cs].astype(F32) + a).astype(BF16)

    for w in (w0, w1, w2, w3, w4, w5, w6, w7, w8, w9):
        w.wait_send()

    osend(0, 1).wait_send()

    @pl.loop(1, npair)
    def _(n):
        osend(n, 0).wait_send()
        osend(n, 1).wait_send()
    for s in pend:
        s.wait_send()


def moe_kernel(cp, tp, cap, h_ref, prow_ref, gates_ref, wg_hbm, wu_hbm, wd_hbm, y_ref,
               sendb, recvb, zb, back, wg, wu, wd, acc, colb, wsem, dss, drs, bss, brs):
    c = lax.axis_index('cp')
    t = lax.axis_index('tp')
    ne = cp * tp
    T, H = h_ref.shape
    grp = 4
    ng = ne // grp
    wc = [pltpu.make_async_copy(a.at[0], b, wsem.at[n]) for n, (a, b) in enumerate(((wg_hbm, wg), (wu_hbm, wu), (wd_hbm, wd)))]
    for w in wc:
        w.start()

    nx = tp // 2
    i, k = t // 2, t % 2

    def offset(d):
        w = d // 2
        return w % cp, (w + w // cp) % nx, d % 2

    def fwd(d):
        dc, di, dk = offset(d)
        return {'cp': (c + dc) % cp, 'tp': ((i + di) % nx) * 2 + (k + dk) % 2}

    def bwd(d):
        dc, di, dk = offset(d)
        return {'cp': (c + cp - dc) % cp, 'tp': ((i + nx - di) % nx) * 2 + (k + dk) % 2}

    b = pltpu.get_barrier_semaphore()

    @pl.loop(1, ne)
    def _(d):
        pl.semaphore_signal(b, inc=1, device_id=fwd(d), device_id_type=MESH)

    def pack(g):
        s = lax.broadcasted_iota(jnp.int32, (grp * cap, T), 0) + g * (grp * cap)
        pick = jnp.where((s == prow_ref[0:1, :]) | (s == prow_ref[1:2, :]), 1.0, 0.0).astype(BF16)
        r = jnp.dot(pick, h_ref[...], preferred_element_type=F32).astype(BF16)
        sendb[pl.ds(g * grp, grp)] = r.reshape(grp, cap, H)

    def disp(d):
        return remote(sendb.at[d], recvb.at[d], dss.at[d], drs.at[d], fwd(d))

    def ret(d):
        return remote(zb.at[d], back.at[d], bss.at[d], brs.at[d], bwd(d))

    pack(0)
    recvb[0] = sendb[0]
    pl.semaphore_wait(b, ne - 1)
    for d in range(1, grp):
        disp(d).start()

    @pl.loop(1, ng)
    def _(g):
        pack(g)
        for j in range(grp):
            disp(g * grp + j).start()

    rows4 = jnp.concatenate([prow_ref[...].astype(F32), gates_ref[...], jnp.zeros((HEAD - 4, T), F32)], axis=0)
    colb[...] = rows4.T
    for w in wc:
        w.wait()

    def ffn(g):
        rows = recvb[pl.ds(g * grp, grp)].reshape(grp * cap, H)
        gg = jnp.dot(rows, wg[...], preferred_element_type=F32)
        uu = jnp.dot(rows, wu[...], preferred_element_type=F32)
        act = (gg * jax.nn.sigmoid(gg) * uu).astype(BF16)
        z = jnp.dot(act, wd[...], preferred_element_type=F32).astype(BF16)
        zb[pl.ds(g * grp, grp)] = z.reshape(grp, cap, H)

    def combine(g):
        zz = back[pl.ds(g * grp, grp)].reshape(grp * cap, H)
        s = lax.broadcasted_iota(jnp.int32, (T, grp * cap), 1) + g * (grp * cap)
        g0 = jnp.where(s == colb[:, 0:1].astype(jnp.int32), 1.0, 0.0).astype(BF16)
        g1 = jnp.where(s == colb[:, 1:2].astype(jnp.int32), 1.0, 0.0).astype(BF16)
        return (colb[:, 2:3] * jnp.dot(g0, zz, preferred_element_type=F32)
                + colb[:, 3:4] * jnp.dot(g1, zz, preferred_element_type=F32))

    for d in range(1, grp):
        disp(d).wait_recv()
    ffn(0)
    back[0] = zb[0]
    for d in range(1, grp):
        ret(d).start()

    @pl.loop(1, ng)
    def _(g):
        for j in range(grp):
            disp(g * grp + j).wait_recv()
        ffn(g)
        for j in range(grp):
            ret(g * grp + j).start()

    for d in range(1, grp):
        ret(d).wait_recv()
    acc[...] = h_ref[...].astype(F32) + combine(0)

    @pl.loop(1, ng)
    def _(g):
        for j in range(grp):
            ret(g * grp + j).wait_recv()
        acc[...] += combine(g)

    y_ref[...] = acc[...].astype(BF16)

    @pl.loop(1, ne)
    def _(d):
        disp(d).wait_send()
        ret(d).wait_send()


def params(cid):
    return pltpu.CompilerParams(collective_id=cid, has_side_effects=True, vmem_limit_bytes=60 * 1024 * 1024)


def attention(x, idx, wq, wk, wv, wo, cp, tp, cap):
    T, H = x.shape
    nx = tp // 2
    nb = cp * tp
    W = wq.shape[1]
    return pl.pallas_call(
        functools.partial(attn_kernel, cp, nx, cap),
        out_shape=[
            jax.ShapeDtypeStruct((T, H), BF16), jax.ShapeDtypeStruct((2, T), jnp.int32),
        ],
        in_specs=[spec(VMEM)] * 6,
        out_specs=[spec(VMEM)] * 2,
        scratch_shapes=[
            VMEM((nb, 3, T, HEAD), BF16), VMEM((3, H, W), BF16), VMEM((3, T, H), BF16), VMEM((7, 4, 3, T, HEAD), BF16),
            VMEM((nb // 2, HEAD, 2 * T), BF16), VMEM((tp, wo.shape[0], H), BF16),
            VMEM((2 * cp, 2, T, HEAD), BF16), VMEM((tp, T, 2 * HEAD), BF16),
            VMEM((2 * T, 2 * T), F32), VMEM((2 * T, 2 * T), F32), VMEM((HEAD, 2 * T), F32),
            DMA((3,)), DMA((3,)), DMA((6,)), DMA((6,)),
            DMA((7, cp)), DMA((7, cp)), DMA((7, cp)), DMA((7, cp)), DMA((7,)),
            DMA((10,)), DMA((10,)), DMA((2 * cp, 2)), DMA((2 * cp, 2)), DMA((2,)),
        ],
        compiler_params=params(0),
        name='attn',
    )(x, wq, wk, wv, wo, idx.T)


def experts(h, prow, gates, w1g, w1u, w2, cp, tp, cap):
    T, H = h.shape
    F = w1g.shape[2]
    ne = cp * tp
    return pl.pallas_call(
        functools.partial(moe_kernel, cp, tp, cap),
        out_shape=jax.ShapeDtypeStruct((T, H), BF16),
        in_specs=[spec(VMEM)] * 3 + [spec(pl.ANY)] * 3,
        out_specs=spec(VMEM),
        scratch_shapes=[VMEM((ne, cap, H), BF16)] * 4 + [
            VMEM((H, F), BF16), VMEM((H, F), BF16), VMEM((F, H), BF16), VMEM((T, H), F32), VMEM((T, HEAD), F32),
            DMA((3,)), DMA((ne,)), DMA((ne,)), DMA((ne,)), DMA((ne,)),
        ],
        compiler_params=params(1),
        name='moe',
    )(h, prow, gates.T, w1g, w1u, w2)


def solution(mesh):
    cp = mesh.shape['cp']
    tp = mesh.shape['tp']
    rows_spec = P(('dp', 'cp', 'tp'), None)
    exp_spec = P(('cp', 'tp'), None, None)

    def local(x, idx, gates, wq, wk, wv, wo, w1g, w1u, w2):
        cap = 4 * x.shape[0] // (cp * tp)
        h, prow = attention(x, idx, wq, wk, wv, wo, cp, tp, cap)
        return experts(h, prow, gates, w1g, w1u, w2, cp, tp, cap)

    return jax.shard_map(local, mesh=mesh, in_specs=(rows_spec, rows_spec, rows_spec, P(None, 'tp'), P(None, 'tp'), P(None, 'tp'), P('tp', None), exp_spec, exp_spec, exp_spec), out_specs=rows_spec, check_vma=False)
```

```python
import functools
import math

import jax
import jax.numpy as jnp
from jax import lax
from jax.experimental import pallas as pl
from jax.experimental.pallas import tpu as pltpu
from jax.sharding import PartitionSpec as P

HEAD = 128
MESH = pl.DeviceIdType.MESH
VMEM = pltpu.VMEM
DMA = pltpu.SemaphoreType.DMA
BF16 = jnp.bfloat16
F32 = jnp.float32


def spec(space):
    return pl.BlockSpec(memory_space=space)


def remote(src, dst, ssem, rsem, dev):
    return pltpu.make_async_remote_copy(src_ref=src, dst_ref=dst, send_sem=ssem, recv_sem=rsem, device_id=dev, device_id_type=MESH)


def barrier_with(devs):
    b = pltpu.get_barrier_semaphore()
    for d in devs:
        pl.semaphore_signal(b, inc=1, device_id=d, device_id_type=MESH)
    pl.semaphore_wait(b, len(devs))


def place(c, chip, core, cp):
    high = chip // 2
    seg = c * (1 - high) + (2 * cp - 1 - c) * high
    return seg * 4 + (chip % 2) * 2 + core


def slots(cp, nx, cap, c, i, k, idx_ref, prow_ref):
    T = idx_ref.shape[1]
    tp = 2 * nx
    ne = cp * tp
    sh = tp.bit_length() - 1
    e = idx_ref[...]
    dc = ((e >> sh) - c) & (cp - 1)
    di = (((e & (tp - 1)) >> 1) - i) & (nx - 1)
    dk = (e - k) & 1
    rel = ((((di - dc) & (nx - 1)) * cp + dc) * 2 + dk)
    experts_i = lax.broadcasted_iota(jnp.int32, (ne, T), 0)
    o0 = (rel[0:1, :] == experts_i).astype(F32)
    o1 = (rel[1:2, :] == experts_i).astype(F32)
    low = lax.broadcasted_iota(jnp.int32, (T, T), 0) < lax.broadcasted_iota(jnp.int32, (T, T), 1)
    prev = jnp.dot((o0 + o1).astype(BF16), low.astype(F32).astype(BF16), preferred_element_type=F32)
    p0 = rel[0:1, :] * cap + jnp.sum(prev * o0, axis=0, keepdims=True).astype(jnp.int32)
    p1 = rel[1:2, :] * cap + jnp.sum(prev * o1, axis=0, keepdims=True).astype(jnp.int32)
    prow_ref[0:1, :] = p0
    prow_ref[1:2, :] = p1


def attn_kernel(cp, nx, cap, x_ref, wq_ref, wk_ref, wv_ref, wo_ref, idx_ref, h_ref, prow_ref,
                kvq, wown, wsib, xb, stage, vt, wof, ostage, obuf, sa, sb, acc,
                wls, wss, wrs, xss, xrs, ass, ars, rss, rrs, qls, wos, wor, oss, ors, ls):
    c = lax.axis_index('cp')
    t = lax.axis_index('tp')
    i, k = t // 2, t % 2
    T, H = x_ref.shape
    sib = {'cp': c, 'tp': i * 2 + 1 - k}
    right = {'cp': c, 'tp': ((i + 1) % nx) * 2 + k}
    left = {'cp': c, 'tp': ((i + nx - 1) % nx) * 2 + k}
    peer = [{'cp': (c + d) % cp, 'tp': t} for d in range(cp)]
    same = [{'cp': (c + dc) % cp, 'tp': ((i + di) % nx) * 2 + k} for di in range(nx) for dc in range(cp)]
    barrier_with([sib] + same[1:])
    full = pl.ds(0, T)

    R = wo_ref.shape[0]
    hr = R // 2
    rlo, rhi, rfull = pl.ds(0, hr), pl.ds(hr, hr), pl.ds(0, R)
    ri, li, oi = (i + 1) % nx, (i + nx - 1) % nx, (i + 2) % nx
    def wcopy(n, src, chip, core, rows, to):
        return remote(src, wof.at[chip * 2 + core, rows], wos.at[n], wor.at[n], to)

    w0 = wcopy(0, wo_ref.at[rlo], i, k, rlo, right)
    w1 = wcopy(1, wo_ref.at[rhi], i, k, rhi, left)
    w2 = wcopy(2, wo_ref.at[rhi], i, k, rhi, right)
    w3 = wcopy(3, wo_ref.at[rlo], i, k, rlo, left)
    w6 = wcopy(6, wo_ref, i, k, rfull, sib)
    wl = pltpu.make_async_copy(wo_ref, wof.at[t], ls.at[0])
    w4 = wcopy(4, wof.at[li * 2 + k, rlo], li, k, rlo, right)
    w5 = wcopy(5, wof.at[ri * 2 + k, rhi], ri, k, rhi, left)
    w7 = wcopy(7, wof.at[li * 2 + k], li, k, rfull, sib)
    w8 = wcopy(8, wof.at[ri * 2 + k], ri, k, rfull, sib)
    w9 = wcopy(9, wof.at[oi * 2 + k], oi, k, rfull, sib)


    quarter = T // 4

    def part(a, b):
        return pl.ds(a * quarter, (b - a) * quarter)

    def xcopy(n, src, slot, rows, dev):
        return remote(src.at[rows], xb.at[slot, rows], xss.at[n], xrs.at[n], dev)

    to_r = [
        xcopy(0, x_ref, 0, part(0, 2), right), xcopy(1, x_ref, 0, part(2, 3), right), xcopy(2, xb.at[0], 2, part(0, 1), right),
        xcopy(3, x_ref, 0, part(3, 4), right), xcopy(4, xb.at[0], 2, part(1, 2), right),
    ]
    to_l = [
        xcopy(5, x_ref, 1, part(2, 4), left), xcopy(6, x_ref, 1, part(1, 2), left), xcopy(7, xb.at[1], 2, part(2, 3), left),
        xcopy(8, x_ref, 1, part(0, 1), left), xcopy(9, xb.at[1], 2, part(3, 4), left),
    ]
    own_h = [wq_ref, wk_ref, wv_ref]
    wsend = [remote(own_h[n], wsib.at[n], wss.at[n], wrs.at[n], sib) for n in range(3)]
    wload = [pltpu.make_async_copy(own_h[n], wown.at[n], wls.at[n]) for n in range(3)]
    for s in (to_r[0], to_l[0], *wload, *wsend, to_r[1], to_l[1]):
        s.start()

    pend = to_r + to_l + wsend
    arrive = []

    units = [
        (0, full), (nx - 1, part(0, 2)), (1, part(2, 4)), (nx - 1, part(2, 3)), (1, part(1, 2)), (2, part(0, 1)), (2, part(2, 3)),
        (nx - 1, part(3, 4)), (1, part(0, 1)), (2, part(1, 2)), (2, part(3, 4)),
    ]

    def compute(u, src):
        rows = units[u][1]
        xv = src[rows, :]
        for w in range(2):
            for n in range(3):
                if u == 0:
                    (wsend[n].wait_recv if w else wload[n].wait)()
                wref = wown if w == 0 else wsib
                r = jnp.dot(xv, wref[n], preferred_element_type=F32).astype(BF16)
                kk = k if w == 0 else 1 - k
                for m in range(2):
                    stage[2 * kk + m, n, pl.ds(base[u], rows.size), :] = r[:, m * HEAD:(m + 1) * HEAD]

    sizes = [r.size for _, r in units]
    base = [sum(sizes[:u]) for u in range(len(units))]

    def staged(u, a, n):
        return stage.at[a, n, pl.ds(base[u], sizes[u])]

    def block_of(u, d):
        dj, _ = units[u]
        return place((c + cp - d) % cp, (i + dj) % nx, k, cp)

    def send(u):
        rows = units[u][1]
        b = block_of(u, 0)
        for d in range(1, cp):
            cps = remote(staged(u, (c + d) % cp, pl.ds(0, 3)), kvq.at[b, :, rows], ass.at[u, d], ars.at[u, d], peer[d])
            cps.start()
            pend.append(cps)
        lc = pltpu.make_async_copy(staged(u, c, pl.ds(0, 3)), kvq.at[b, :, rows], qls.at[u])
        lc.start()
        locs.append(lc)
        relay(u, 0, staged(u, c, pl.ds(1, 2)))

    def relay(u, d, src):
        rows = units[u][1]
        b = block_of(u, d)
        cps = remote(src, kvq.at[b, pl.ds(1, 2), rows], rss.at[u, d], rrs.at[u, d], sib)
        cps.start()
        pend.append(cps)
        arrive.append((u, d))

    def pass_on(u):
        rows = units[u][1]
        for d in range(1, cp):
            b = block_of(u, d)
            remote(staged(u, 0, pl.ds(0, 3)), kvq.at[b, :, rows], ass.at[u, d], ars.at[u, d], peer[d]).wait_recv()
            relay(u, d, kvq.at[b, pl.ds(1, 2), rows])

    locs = []
    compute(0, x_ref)
    send(0)
    slots(cp, nx, cap, c, i, k, idx_ref, prow_ref)
    for first, rest in ((to_r[0], to_r[2:]), (to_l[0], to_l[2:])):
        first.wait_recv()
        for s in rest:
            s.start()
    for w in (w0, w1, w2, w3, w6):
        w.start()
    wl.start()
    for u, src, got in ((1, 0, None), (2, 1, None), (3, 0, to_r[1]), (4, 1, to_l[1]), (5, 2, to_r[2]), (6, 2, to_l[2]),
                        (7, 0, to_r[3]), (8, 1, to_l[3]), (9, 2, to_r[4]), (10, 2, to_l[4])):
        if got is not None:
            got.wait_recv()
        compute(u, xb.at[src])
        send(u)
        for v in {2: (0,), 4: (1, 2), 6: (3, 4), 8: (5, 6)}.get(u, ()):
            pass_on(v)
    for u in range(7, 11):
        pass_on(u)
    for u, d in arrive:
        rows = units[u][1]
        b = block_of(u, d) + 1 - 2 * k
        remote(staged(u, 0, pl.ds(1, 2)), kvq.at[b, pl.ds(1, 2), rows], rss.at[u, d], rrs.at[u, d], sib).wait_recv()
    for lc in locs:
        lc.wait()

    w0.wait_recv()
    w4.start()
    w1.wait_recv()
    w5.start()
    nch = kvq.shape[0] // 2

    @pl.loop(0, nch)
    def _(m):
        v = kvq[pl.ds(2 * m, 2), 2].reshape(2 * T, HEAD)
        vt[m] = v.astype(F32).T.astype(BF16)

    scale = HEAD ** -0.5 * math.log2(math.e)
    par = i % 2
    col_i = lax.broadcasted_iota(jnp.int32, (1, 2 * T), 1)
    qpos = col_i % T + k * T + 2 * T * jnp.where(col_i < T, par, 1 - par)
    row_i = lax.broadcasted_iota(jnp.int32, (2 * T, 2 * T), 0)

    def scores(q, m, part, buf):
        kb = kvq[pl.ds(2 * m, 2), 1].reshape(2 * T, HEAD)
        s = lax.dot_general(kb, q, (((1,), (1,)), ((), ())), preferred_element_type=F32)
        if part is not None:
            s = jnp.where(row_i + 2 * T * part <= qpos, s, -jnp.inf)
        buf[...] = s
        return jnp.max(s, axis=0, keepdims=True)

    def absorb(buf, m, top, ml):
        mo, l = ml
        mn = jnp.maximum(mo, top)
        w = jnp.exp2((buf[...] - mn) * scale)
        a = jnp.exp2((mo - mn) * scale)
        l = l * a + jnp.sum(w, axis=0, keepdims=True)
        acc[...] = acc[...] * a + jnp.dot(vt[m], w.astype(BF16), preferred_element_type=F32)
        return mn, l

    def attend(n):
        cc = (c + n % cp) % cp
        high = (i // 2 + n // cp) % 2
        pb0 = place(cc, 2 * high + par, k, cp)
        pb1 = place(cc, 2 * high + 1 - par, k, cp)
        q = jnp.concatenate([kvq[pb0, 0], kvq[pb1, 0]], axis=0)
        p = pb0 // 4
        acc[...] = jnp.zeros_like(acc)
        last = p * 2

        def body(j, carry):
            ml, ta = carry
            tb = scores(q, 2 * j + 1, None, sb)
            ml = absorb(sa, 2 * j, ta, ml)
            ta = scores(q, 2 * j + 2, None, sa)
            return absorb(sb, 2 * j + 1, tb, ml), ta

        ml = (jnp.full((1, 2 * T), -jnp.inf, F32), jnp.zeros((1, 2 * T), F32))
        ta = scores(q, 0, None, sa)
        ml, ta = lax.fori_loop(0, p, body, (ml, ta))
        s = jnp.where(row_i <= qpos, sa[...], -jnp.inf)
        sa[...] = s
        ta = jnp.max(s, axis=0, keepdims=True)
        tb = scores(q, last + 1, 1, sb)
        ml = absorb(sa, last, ta, ml)
        _, l = absorb(sb, last + 1, tb, ml)
        o = (acc[...] / l).T.astype(BF16)
        ostage[n, 0] = o[:T]
        ostage[n, 1] = o[T:]

    col = pl.ds((c % 2) * HEAD, HEAD)
    npair = 2 * cp

    def owner(n, e, sign):
        chip = 2 * ((i // 2 + n // cp) % 2) + (par + e) % 2
        return {'cp': (c + sign * (n % cp) + cp) % cp, 'tp': chip * 2 + k}

    def osend(n, e):
        return remote(ostage.at[n, e], obuf.at[i * 2 + c // 2, :, col], oss.at[n, e], ors.at[n, e], owner(n, e, 1))

    def run(a, b):
        @pl.loop(a, b)
        def _(n):
            attend(n)
            osend(n, 0).start()
            osend(n, 1).start()

    run(1, 4)
    w2.wait_recv()
    w7.start()
    w3.wait_recv()
    w8.start()
    run(4, npair)
    attend(0)
    osend(0, 1).start()
    lo_c = pltpu.make_async_copy(ostage.at[0, 0], obuf.at[i * 2 + c // 2, :, col], ls.at[1])
    lo_c.start()
    w4.wait_recv()
    w5.wait_recv()
    w9.start()
    wl.wait()
    for w in (w6, w7, w8, w9):
        w.wait_recv()
    lo_c.wait()
    osend(0, 1).wait_recv()

    @pl.loop(1, npair)
    def _(n):
        osend(n, 0).wait_recv()
        osend(n, 1).wait_recv()

    nt = wof.shape[0]
    cw = min(512, H)
    for j in range(H // cw):
        cs = slice(j * cw, (j + 1) * cw)
        a = jnp.dot(obuf[0], wof[0, :, cs], preferred_element_type=F32)
        for tt in range(1, nt):
            a += jnp.dot(obuf[tt], wof[tt, :, cs], preferred_element_type=F32)
        h_ref[:, cs] = (x_ref[:, cs].astype(F32) + a).astype(BF16)

    for w in (w0, w1, w2, w3, w4, w5, w6, w7, w8, w9):
        w.wait_send()

    osend(0, 1).wait_send()

    @pl.loop(1, npair)
    def _(n):
        osend(n, 0).wait_send()
        osend(n, 1).wait_send()
    for s in pend:
        s.wait_send()


def moe_kernel(cp, tp, cap, h_ref, prow_ref, gates_ref, wg_hbm, wu_hbm, wd_hbm, y_ref,
               sendb, recvb, zb, back, wg, wu, wd, acc, colb, wsem, dss, drs, bss, brs):
    c = lax.axis_index('cp')
    t = lax.axis_index('tp')
    ne = cp * tp
    T, H = h_ref.shape
    grp = 4
    ng = ne // grp
    wc = [pltpu.make_async_copy(a.at[0], b, wsem.at[n]) for n, (a, b) in enumerate(((wg_hbm, wg), (wu_hbm, wu), (wd_hbm, wd)))]
    for w in wc:
        w.start()

    nx = tp // 2
    i, k = t // 2, t % 2

    def offset(d):
        w = d // 2
        return w % cp, (w + w // cp) % nx, d % 2

    def fwd(d):
        dc, di, dk = offset(d)
        return {'cp': (c + dc) % cp, 'tp': ((i + di) % nx) * 2 + (k + dk) % 2}

    def bwd(d):
        dc, di, dk = offset(d)
        return {'cp': (c + cp - dc) % cp, 'tp': ((i + nx - di) % nx) * 2 + (k + dk) % 2}

    b = pltpu.get_barrier_semaphore()

    @pl.loop(1, ne)
    def _(d):
        pl.semaphore_signal(b, inc=1, device_id=fwd(d), device_id_type=MESH)

    def pack(g):
        s = lax.broadcasted_iota(jnp.int32, (grp * cap, T), 0) + g * (grp * cap)
        pick = jnp.where((s == prow_ref[0:1, :]) | (s == prow_ref[1:2, :]), 1.0, 0.0).astype(BF16)
        r = jnp.dot(pick, h_ref[...], preferred_element_type=F32).astype(BF16)
        sendb[pl.ds(g * grp, grp)] = r.reshape(grp, cap, H)

    def disp(d):
        return remote(sendb.at[d], recvb.at[d], dss.at[d], drs.at[d], fwd(d))

    def ret(d):
        return remote(zb.at[d], back.at[d], bss.at[d], brs.at[d], bwd(d))

    pack(0)
    recvb[0] = sendb[0]
    pl.semaphore_wait(b, ne - 1)
    for d in range(1, grp):
        disp(d).start()

    @pl.loop(1, ng)
    def _(g):
        pack(g)
        for j in range(grp):
            disp(g * grp + j).start()

    rows4 = jnp.concatenate([prow_ref[...].astype(F32), gates_ref[...], jnp.zeros((HEAD - 4, T), F32)], axis=0)
    colb[...] = rows4.T
    for w in wc:
        w.wait()

    def ffn(g):
        rows = recvb[pl.ds(g * grp, grp)].reshape(grp * cap, H)
        gg = jnp.dot(rows, wg[...], preferred_element_type=F32)
        uu = jnp.dot(rows, wu[...], preferred_element_type=F32)
        act = (gg * jax.nn.sigmoid(gg) * uu).astype(BF16)
        z = jnp.dot(act, wd[...], preferred_element_type=F32).astype(BF16)
        zb[pl.ds(g * grp, grp)] = z.reshape(grp, cap, H)

    def combine(g):
        zz = back[pl.ds(g * grp, grp)].reshape(grp * cap, H)
        s = lax.broadcasted_iota(jnp.int32, (T, grp * cap), 1) + g * (grp * cap)
        g0 = jnp.where(s == colb[:, 0:1].astype(jnp.int32), 1.0, 0.0).astype(BF16)
        g1 = jnp.where(s == colb[:, 1:2].astype(jnp.int32), 1.0, 0.0).astype(BF16)
        return (colb[:, 2:3] * jnp.dot(g0, zz, preferred_element_type=F32)
                + colb[:, 3:4] * jnp.dot(g1, zz, preferred_element_type=F32))

    for d in range(1, grp):
        disp(d).wait_recv()
    ffn(0)
    back[0] = zb[0]
    for d in range(1, grp):
        ret(d).start()

    @pl.loop(1, ng)
    def _(g):
        for j in range(grp):
            disp(g * grp + j).wait_recv()
        ffn(g)
        for j in range(grp):
            ret(g * grp + j).start()

    for d in range(1, grp):
        ret(d).wait_recv()
    acc[...] = h_ref[...].astype(F32) + combine(0)

    @pl.loop(1, ng)
    def _(g):
        for j in range(grp):
            ret(g * grp + j).wait_recv()
        acc[...] += combine(g)

    y_ref[...] = acc[...].astype(BF16)

    @pl.loop(1, ne)
    def _(d):
        disp(d).wait_send()
        ret(d).wait_send()


def params(cid):
    return pltpu.CompilerParams(collective_id=cid, has_side_effects=True, vmem_limit_bytes=60 * 1024 * 1024)


def attention(x, idx, wq, wk, wv, wo, cp, tp, cap):
    T, H = x.shape
    nx = tp // 2
    nb = cp * tp
    W = wq.shape[1]
    return pl.pallas_call(
        functools.partial(attn_kernel, cp, nx, cap),
        out_shape=[
            jax.ShapeDtypeStruct((T, H), BF16), jax.ShapeDtypeStruct((2, T), jnp.int32),
        ],
        in_specs=[spec(VMEM)] + [spec(pl.ANY)] * 4 + [spec(VMEM)],
        out_specs=[spec(VMEM)] * 2,
        scratch_shapes=[
            VMEM((nb, 3, T, HEAD), BF16), VMEM((3, H, W), BF16), VMEM((3, H, W), BF16), VMEM((3, T, H), BF16), VMEM((4, 3, nx * T, HEAD), BF16),
            VMEM((nb // 2, HEAD, 2 * T), BF16), VMEM((tp, wo.shape[0], H), BF16),
            VMEM((2 * cp, 2, T, HEAD), BF16), VMEM((tp, T, 2 * HEAD), BF16),
            VMEM((2 * T, 2 * T), F32), VMEM((2 * T, 2 * T), F32), VMEM((HEAD, 2 * T), F32),
            DMA((3,)), DMA((3,)), DMA((3,)), DMA((10,)), DMA((10,)),
            DMA((11, cp)), DMA((11, cp)), DMA((11, cp)), DMA((11, cp)), DMA((11,)),
            DMA((10,)), DMA((10,)), DMA((2 * cp, 2)), DMA((2 * cp, 2)), DMA((2,)),
        ],
        compiler_params=params(0),
        name='attn',
    )(x, wq, wk, wv, wo, idx.T)


def experts(h, prow, gates, w1g, w1u, w2, cp, tp, cap):
    T, H = h.shape
    F = w1g.shape[2]
    ne = cp * tp
    return pl.pallas_call(
        functools.partial(moe_kernel, cp, tp, cap),
        out_shape=jax.ShapeDtypeStruct((T, H), BF16),
        in_specs=[spec(VMEM)] * 3 + [spec(pl.ANY)] * 3,
        out_specs=spec(VMEM),
        scratch_shapes=[VMEM((ne, cap, H), BF16)] * 4 + [
            VMEM((H, F), BF16), VMEM((H, F), BF16), VMEM((F, H), BF16), VMEM((T, H), F32), VMEM((T, HEAD), F32),
            DMA((3,)), DMA((ne,)), DMA((ne,)), DMA((ne,)), DMA((ne,)),
        ],
        compiler_params=params(1),
        name='moe',
    )(h, prow, gates.T, w1g, w1u, w2)


def solution(mesh):
    cp = mesh.shape['cp']
    tp = mesh.shape['tp']
    rows_spec = P(('dp', 'cp', 'tp'), None)
    exp_spec = P(('cp', 'tp'), None, None)

    def local(x, idx, gates, wq, wk, wv, wo, w1g, w1u, w2):
        cap = 4 * x.shape[0] // (cp * tp)
        h, prow = attention(x, idx, wq, wk, wv, wo, cp, tp, cap)
        return experts(h, prow, gates, w1g, w1u, w2, cp, tp, cap)

    return jax.shard_map(local, mesh=mesh, in_specs=(rows_spec, rows_spec, rows_spec, P(None, 'tp'), P(None, 'tp'), P(None, 'tp'), P('tp', None), exp_spec, exp_spec, exp_spec), out_specs=rows_spec, check_vma=False)
```

```python
import functools
import math

import jax
import jax.numpy as jnp
from jax import lax
from jax.experimental import pallas as pl
from jax.experimental.pallas import tpu as pltpu
from jax.sharding import PartitionSpec as P

HEAD = 128
MESH = pl.DeviceIdType.MESH
VMEM = pltpu.VMEM
DMA = pltpu.SemaphoreType.DMA
BF16 = jnp.bfloat16
F32 = jnp.float32


def spec(space):
    return pl.BlockSpec(memory_space=space)


def remote(src, dst, ssem, rsem, dev):
    return pltpu.make_async_remote_copy(src_ref=src, dst_ref=dst, send_sem=ssem, recv_sem=rsem, device_id=dev, device_id_type=MESH)


def barrier_with(devs):
    b = pltpu.get_barrier_semaphore()
    for d in devs:
        pl.semaphore_signal(b, inc=1, device_id=d, device_id_type=MESH)
    pl.semaphore_wait(b, len(devs))


def place(c, chip, core, cp):
    high = chip // 2
    seg = c * (1 - high) + (2 * cp - 1 - c) * high
    return seg * 4 + (chip % 2) * 2 + core


def slots(cp, nx, cap, c, i, k, idx_ref, prow_ref):
    T = idx_ref.shape[1]
    tp = 2 * nx
    ne = cp * tp
    sh = tp.bit_length() - 1
    e = idx_ref[...]
    dc = ((e >> sh) - c) & (cp - 1)
    di = (((e & (tp - 1)) >> 1) - i) & (nx - 1)
    dk = (e - k) & 1
    rel = ((((di - dc) & (nx - 1)) * cp + dc) * 2 + dk)
    experts_i = lax.broadcasted_iota(jnp.int32, (ne, T), 0)
    o0 = (rel[0:1, :] == experts_i).astype(F32)
    o1 = (rel[1:2, :] == experts_i).astype(F32)
    low = lax.broadcasted_iota(jnp.int32, (T, T), 0) < lax.broadcasted_iota(jnp.int32, (T, T), 1)
    prev = jnp.dot((o0 + o1).astype(BF16), low.astype(F32).astype(BF16), preferred_element_type=F32)
    p0 = rel[0:1, :] * cap + jnp.sum(prev * o0, axis=0, keepdims=True).astype(jnp.int32)
    p1 = rel[1:2, :] * cap + jnp.sum(prev * o1, axis=0, keepdims=True).astype(jnp.int32)
    prow_ref[0:1, :] = p0
    prow_ref[1:2, :] = p1


def attn_kernel(cp, nx, cap, x_ref, wq_ref, wk_ref, wv_ref, wo_ref, idx_ref, h_ref, prow_ref,
                kvq, wown, wsib, xb, stage, vt, wof, ostage, obuf, sa, sb, acc,
                wls, wss, wrs, xss, xrs, ass, ars, rss, rrs, qls, wos, wor, oss, ors, ls, bxs, bxr, bys, byr):
    c = lax.axis_index('cp')
    t = lax.axis_index('tp')
    i, k = t // 2, t % 2
    T, H = x_ref.shape
    sib = {'cp': c, 'tp': i * 2 + 1 - k}
    right = {'cp': c, 'tp': ((i + 1) % nx) * 2 + k}
    left = {'cp': c, 'tp': ((i + nx - 1) % nx) * 2 + k}
    peer = [{'cp': (c + d) % cp, 'tp': t} for d in range(cp)]
    same = [{'cp': (c + dc) % cp, 'tp': ((i + di) % nx) * 2 + k} for di in range(nx) for dc in range(cp)]
    barrier_with([sib] + same[1:])
    full = pl.ds(0, T)

    R = wo_ref.shape[0]
    hr = R // 4
    rlo, rhi, rfull = pl.ds(0, hr), pl.ds(hr, hr), pl.ds(0, R)
    ri, li, oi = (i + 1) % nx, (i + nx - 1) % nx, (i + 2) % nx
    def wcopy(n, src, chip, core, rows, to):
        return remote(src, wof.at[chip * 2 + core, rows], wos.at[n], wor.at[n], to)

    w0 = wcopy(0, wo_ref.at[rlo], i, k, rlo, right)
    w1 = wcopy(1, wo_ref.at[rhi], i, k, rhi, left)
    w2 = wcopy(2, wo_ref.at[rhi], i, k, rhi, right)
    w3 = wcopy(3, wo_ref.at[rlo], i, k, rlo, left)
    w6 = wcopy(6, wo_ref, i, k, rfull, sib)
    wl = pltpu.make_async_copy(wo_ref, wof.at[t], ls.at[0])
    w4 = wcopy(4, wof.at[li * 2 + k, rlo], li, k, rlo, right)
    w5 = wcopy(5, wof.at[ri * 2 + k, rhi], ri, k, rhi, left)
    w7 = wcopy(7, wof.at[li * 2 + k], li, k, rfull, sib)
    w8 = wcopy(8, wof.at[ri * 2 + k], ri, k, rfull, sib)
    w9 = wcopy(9, wof.at[oi * 2 + k], oi, k, rfull, sib)


    rq = pl.ds(R // 2 + c * (R // 2 // cp), R // 2 // cp)

    def wrow(di):
        return remote(wo_ref.at[rq], wof.at[t, rq], bxs.at[di], bxr.at[di], {'cp': c, 'tp': ((i + di) % nx) * 2 + k})

    def wcol(di, d):
        shard = ((i + nx - di) % nx) * 2 + k
        return remote(wof.at[shard, rq], wof.at[shard, rq], bys.at[di, d], byr.at[di, d], peer[d])

    quarter = T // 4

    def part(a, b):
        return pl.ds(a * quarter, (b - a) * quarter)

    def xcopy(n, src, slot, rows, dev):
        return remote(src.at[rows], xb.at[slot, rows], xss.at[n], xrs.at[n], dev)

    to_r = [
        xcopy(0, x_ref, 0, part(0, 2), right), xcopy(1, x_ref, 0, part(2, 3), right), xcopy(2, xb.at[0], 2, part(0, 1), right),
        xcopy(3, x_ref, 0, part(3, 4), right), xcopy(4, xb.at[0], 2, part(1, 2), right),
    ]
    to_l = [
        xcopy(5, x_ref, 1, part(2, 4), left), xcopy(6, x_ref, 1, part(1, 2), left), xcopy(7, xb.at[1], 2, part(2, 3), left),
        xcopy(8, x_ref, 1, part(0, 1), left), xcopy(9, xb.at[1], 2, part(3, 4), left),
    ]
    own_h = [wq_ref, wk_ref, wv_ref]
    wsend = [remote(own_h[n], wsib.at[n], wss.at[n], wrs.at[n], sib) for n in range(3)]
    wload = [pltpu.make_async_copy(own_h[n], wown.at[n], wls.at[n]) for n in range(3)]
    for s in (to_r[0], to_l[0], *wload, *wsend, to_r[1], to_l[1]):
        s.start()

    pend = to_r + to_l + wsend
    arrive = []

    units = [
        (0, full), (nx - 1, part(0, 2)), (1, part(2, 4)), (nx - 1, part(2, 3)), (1, part(1, 2)), (2, part(0, 1)), (2, part(2, 3)),
        (nx - 1, part(3, 4)), (1, part(0, 1)), (2, part(1, 2)), (2, part(3, 4)),
    ]

    def compute(u, src):
        rows = units[u][1]
        xv = src[rows, :]
        for w in range(2):
            for n in range(3):
                if u == 0:
                    (wsend[n].wait_recv if w else wload[n].wait)()
                wref = wown if w == 0 else wsib
                r = jnp.dot(xv, wref[n], preferred_element_type=F32).astype(BF16)
                kk = k if w == 0 else 1 - k
                for m in range(2):
                    stage[2 * kk + m, n, pl.ds(base[u], rows.size), :] = r[:, m * HEAD:(m + 1) * HEAD]

    sizes = [r.size for _, r in units]
    base = [sum(sizes[:u]) for u in range(len(units))]

    def staged(u, a, n):
        return stage.at[a, n, pl.ds(base[u], sizes[u])]

    def block_of(u, d):
        dj, _ = units[u]
        return place((c + cp - d) % cp, (i + dj) % nx, k, cp)

    def send(u):
        rows = units[u][1]
        b = block_of(u, 0)
        for d in range(1, cp):
            cps = remote(staged(u, (c + d) % cp, pl.ds(0, 3)), kvq.at[b, :, rows], ass.at[u, d], ars.at[u, d], peer[d])
            cps.start()
            pend.append(cps)
        lc = pltpu.make_async_copy(staged(u, c, pl.ds(0, 3)), kvq.at[b, :, rows], qls.at[u])
        lc.start()
        locs.append(lc)
        relay(u, 0, staged(u, c, pl.ds(1, 2)))

    def relay(u, d, src):
        rows = units[u][1]
        b = block_of(u, d)
        cps = remote(src, kvq.at[b, pl.ds(1, 2), rows], rss.at[u, d], rrs.at[u, d], sib)
        cps.start()
        pend.append(cps)
        arrive.append((u, d))

    def pass_on(u):
        rows = units[u][1]
        for d in range(1, cp):
            b = block_of(u, d)
            remote(staged(u, 0, pl.ds(0, 3)), kvq.at[b, :, rows], ass.at[u, d], ars.at[u, d], peer[d]).wait_recv()
            relay(u, d, kvq.at[b, pl.ds(1, 2), rows])

    locs = []
    compute(0, x_ref)
    send(0)
    slots(cp, nx, cap, c, i, k, idx_ref, prow_ref)
    for first, rest in ((to_r[0], to_r[2:]), (to_l[0], to_l[2:])):
        first.wait_recv()
        for s in rest:
            s.start()
    for w in (wrow(1), wrow(nx - 1), wrow(2), w0, w1, w2, w3, w6):
        w.start()
    wl.start()
    for u, src, got in ((1, 0, None), (2, 1, None), (3, 0, to_r[1]), (4, 1, to_l[1]), (5, 2, to_r[2]), (6, 2, to_l[2]),
                        (7, 0, to_r[3]), (8, 1, to_l[3]), (9, 2, to_r[4]), (10, 2, to_l[4])):
        if got is not None:
            got.wait_recv()
        compute(u, xb.at[src])
        send(u)
        for v in {2: (0,), 4: (1, 2), 6: (3, 4), 8: (5, 6)}.get(u, ()):
            pass_on(v)
    for di in range(1, nx):
        wrow(di).wait_recv()
        for d in range(1, cp):
            wcol(di, d).start()
    for u in range(7, 11):
        pass_on(u)
    for u, d in arrive:
        rows = units[u][1]
        b = block_of(u, d) + 1 - 2 * k
        remote(staged(u, 0, pl.ds(1, 2)), kvq.at[b, pl.ds(1, 2), rows], rss.at[u, d], rrs.at[u, d], sib).wait_recv()
    for lc in locs:
        lc.wait()

    w0.wait_recv()
    w4.start()
    w1.wait_recv()
    w5.start()
    nch = kvq.shape[0] // 2

    @pl.loop(0, nch)
    def _(m):
        v = kvq[pl.ds(2 * m, 2), 2].reshape(2 * T, HEAD)
        vt[m] = v.astype(F32).T.astype(BF16)

    scale = HEAD ** -0.5 * math.log2(math.e)
    par = i % 2
    col_i = lax.broadcasted_iota(jnp.int32, (1, 2 * T), 1)
    qpos = col_i % T + k * T + 2 * T * jnp.where(col_i < T, par, 1 - par)
    row_i = lax.broadcasted_iota(jnp.int32, (2 * T, 2 * T), 0)

    def scores(q, m, part, buf):
        kb = kvq[pl.ds(2 * m, 2), 1].reshape(2 * T, HEAD)
        s = lax.dot_general(kb, q, (((1,), (1,)), ((), ())), preferred_element_type=F32)
        if part is not None:
            s = jnp.where(row_i + 2 * T * part <= qpos, s, -jnp.inf)
        buf[...] = s
        return jnp.max(s, axis=0, keepdims=True)

    def absorb(buf, m, top, ml):
        mo, l = ml
        mn = jnp.maximum(mo, top)
        w = jnp.exp2((buf[...] - mn) * scale)
        a = jnp.exp2((mo - mn) * scale)
        l = l * a + jnp.sum(w, axis=0, keepdims=True)
        acc[...] = acc[...] * a + jnp.dot(vt[m], w.astype(BF16), preferred_element_type=F32)
        return mn, l

    def attend(n):
        cc = (c + n % cp) % cp
        high = (i // 2 + n // cp) % 2
        pb0 = place(cc, 2 * high + par, k, cp)
        pb1 = place(cc, 2 * high + 1 - par, k, cp)
        q = jnp.concatenate([kvq[pb0, 0], kvq[pb1, 0]], axis=0)
        p = pb0 // 4
        acc[...] = jnp.zeros_like(acc)
        last = p * 2

        def body(j, carry):
            ml, ta = carry
            tb = scores(q, 2 * j + 1, None, sb)
            ml = absorb(sa, 2 * j, ta, ml)
            ta = scores(q, 2 * j + 2, None, sa)
            return absorb(sb, 2 * j + 1, tb, ml), ta

        ml = (jnp.full((1, 2 * T), -jnp.inf, F32), jnp.zeros((1, 2 * T), F32))
        ta = scores(q, 0, None, sa)
        ml, ta = lax.fori_loop(0, p, body, (ml, ta))
        s = jnp.where(row_i <= qpos, sa[...], -jnp.inf)
        sa[...] = s
        ta = jnp.max(s, axis=0, keepdims=True)
        tb = scores(q, last + 1, 1, sb)
        ml = absorb(sa, last, ta, ml)
        _, l = absorb(sb, last + 1, tb, ml)
        o = (acc[...] / l).T.astype(BF16)
        ostage[n, 0] = o[:T]
        ostage[n, 1] = o[T:]

    col = pl.ds((c % 2) * HEAD, HEAD)
    npair = 2 * cp

    def owner(n, e, sign):
        chip = 2 * ((i // 2 + n // cp) % 2) + (par + e) % 2
        return {'cp': (c + sign * (n % cp) + cp) % cp, 'tp': chip * 2 + k}

    def osend(n, e):
        return remote(ostage.at[n, e], obuf.at[i * 2 + c // 2, :, col], oss.at[n, e], ors.at[n, e], owner(n, e, 1))

    def run(a, b):
        @pl.loop(a, b)
        def _(n):
            attend(n)
            osend(n, 0).start()
            osend(n, 1).start()

    run(1, 5)
    for di in range(1, nx):
        for d in range(1, cp):
            wcol(di, d).wait_recv()
    for w in (w2, w3, w4, w5):
        w.wait_recv()
    for w in (w7, w8, w9):
        w.start()
    run(5, npair)
    attend(0)
    osend(0, 1).start()
    lo_c = pltpu.make_async_copy(ostage.at[0, 0], obuf.at[i * 2 + c // 2, :, col], ls.at[1])
    lo_c.start()
    wl.wait()
    for w in (w6, w7, w8, w9):
        w.wait_recv()
    lo_c.wait()
    osend(0, 1).wait_recv()

    @pl.loop(1, npair)
    def _(n):
        osend(n, 0).wait_recv()
        osend(n, 1).wait_recv()

    nt = wof.shape[0]
    cw = min(512, H)
    for j in range(H // cw):
        cs = slice(j * cw, (j + 1) * cw)
        a = jnp.dot(obuf[0], wof[0, :, cs], preferred_element_type=F32)
        for tt in range(1, nt):
            a += jnp.dot(obuf[tt], wof[tt, :, cs], preferred_element_type=F32)
        h_ref[:, cs] = (x_ref[:, cs].astype(F32) + a).astype(BF16)

    for w in (w0, w1, w2, w3, w4, w5, w6, w7, w8, w9):
        w.wait_send()
    for di in range(1, nx):
        wrow(di).wait_send()
        for d in range(1, cp):
            wcol(di, d).wait_send()

    osend(0, 1).wait_send()

    @pl.loop(1, npair)
    def _(n):
        osend(n, 0).wait_send()
        osend(n, 1).wait_send()
    for s in pend:
        s.wait_send()


def moe_kernel(cp, tp, cap, h_ref, prow_ref, gates_ref, wg_hbm, wu_hbm, wd_hbm, y_ref,
               sendb, recvb, zb, back, wg, wu, wd, acc, colb, wsem, dss, drs, bss, brs):
    c = lax.axis_index('cp')
    t = lax.axis_index('tp')
    ne = cp * tp
    T, H = h_ref.shape
    grp = 4
    ng = ne // grp
    wc = [pltpu.make_async_copy(a.at[0], b, wsem.at[n]) for n, (a, b) in enumerate(((wg_hbm, wg), (wu_hbm, wu), (wd_hbm, wd)))]
    for w in wc:
        w.start()

    nx = tp // 2
    i, k = t // 2, t % 2

    def offset(d):
        w = d // 2
        return w % cp, (w + w // cp) % nx, d % 2

    def fwd(d):
        dc, di, dk = offset(d)
        return {'cp': (c + dc) % cp, 'tp': ((i + di) % nx) * 2 + (k + dk) % 2}

    def bwd(d):
        dc, di, dk = offset(d)
        return {'cp': (c + cp - dc) % cp, 'tp': ((i + nx - di) % nx) * 2 + (k + dk) % 2}

    b = pltpu.get_barrier_semaphore()

    @pl.loop(1, ne)
    def _(d):
        pl.semaphore_signal(b, inc=1, device_id=fwd(d), device_id_type=MESH)

    def pack(g):
        s = lax.broadcasted_iota(jnp.int32, (grp * cap, T), 0) + g * (grp * cap)
        pick = jnp.where((s == prow_ref[0:1, :]) | (s == prow_ref[1:2, :]), 1.0, 0.0).astype(BF16)
        r = jnp.dot(pick, h_ref[...], preferred_element_type=F32).astype(BF16)
        sendb[pl.ds(g * grp, grp)] = r.reshape(grp, cap, H)

    def disp(d):
        return remote(sendb.at[d], recvb.at[d], dss.at[d], drs.at[d], fwd(d))

    def ret(d):
        return remote(zb.at[d], back.at[d], bss.at[d], brs.at[d], bwd(d))

    pack(0)
    recvb[0] = sendb[0]
    pl.semaphore_wait(b, ne - 1)
    for d in range(1, grp):
        disp(d).start()

    @pl.loop(1, ng)
    def _(g):
        pack(g)
        for j in range(grp):
            disp(g * grp + j).start()

    rows4 = jnp.concatenate([prow_ref[...].astype(F32), gates_ref[...], jnp.zeros((HEAD - 4, T), F32)], axis=0)
    colb[...] = rows4.T
    for w in wc:
        w.wait()

    def ffn(g):
        rows = recvb[pl.ds(g * grp, grp)].reshape(grp * cap, H)
        gg = jnp.dot(rows, wg[...], preferred_element_type=F32)
        uu = jnp.dot(rows, wu[...], preferred_element_type=F32)
        act = (gg * jax.nn.sigmoid(gg) * uu).astype(BF16)
        z = jnp.dot(act, wd[...], preferred_element_type=F32).astype(BF16)
        zb[pl.ds(g * grp, grp)] = z.reshape(grp, cap, H)

    def combine(g):
        zz = back[pl.ds(g * grp, grp)].reshape(grp * cap, H)
        s = lax.broadcasted_iota(jnp.int32, (T, grp * cap), 1) + g * (grp * cap)
        g0 = jnp.where(s == colb[:, 0:1].astype(jnp.int32), 1.0, 0.0).astype(BF16)
        g1 = jnp.where(s == colb[:, 1:2].astype(jnp.int32), 1.0, 0.0).astype(BF16)
        return (colb[:, 2:3] * jnp.dot(g0, zz, preferred_element_type=F32)
                + colb[:, 3:4] * jnp.dot(g1, zz, preferred_element_type=F32))

    for d in range(1, grp):
        disp(d).wait_recv()
    ffn(0)
    back[0] = zb[0]
    for d in range(1, grp):
        ret(d).start()

    @pl.loop(1, ng)
    def _(g):
        for j in range(grp):
            disp(g * grp + j).wait_recv()
        ffn(g)
        for j in range(grp):
            ret(g * grp + j).start()

    for d in range(1, grp):
        ret(d).wait_recv()
    acc[...] = h_ref[...].astype(F32) + combine(0)

    @pl.loop(1, ng)
    def _(g):
        for j in range(grp):
            ret(g * grp + j).wait_recv()
        acc[...] += combine(g)

    y_ref[...] = acc[...].astype(BF16)

    @pl.loop(1, ne)
    def _(d):
        disp(d).wait_send()
        ret(d).wait_send()


def params(cid):
    return pltpu.CompilerParams(collective_id=cid, has_side_effects=True, vmem_limit_bytes=60 * 1024 * 1024)


def attention(x, idx, wq, wk, wv, wo, cp, tp, cap):
    T, H = x.shape
    nx = tp // 2
    nb = cp * tp
    W = wq.shape[1]
    return pl.pallas_call(
        functools.partial(attn_kernel, cp, nx, cap),
        out_shape=[
            jax.ShapeDtypeStruct((T, H), BF16), jax.ShapeDtypeStruct((2, T), jnp.int32),
        ],
        in_specs=[spec(VMEM)] + [spec(pl.ANY)] * 4 + [spec(VMEM)],
        out_specs=[spec(VMEM)] * 2,
        scratch_shapes=[
            VMEM((nb, 3, T, HEAD), BF16), VMEM((3, H, W), BF16), VMEM((3, H, W), BF16), VMEM((3, T, H), BF16), VMEM((4, 3, nx * T, HEAD), BF16),
            VMEM((nb // 2, HEAD, 2 * T), BF16), VMEM((tp, wo.shape[0], H), BF16),
            VMEM((2 * cp, 2, T, HEAD), BF16), VMEM((tp, T, 2 * HEAD), BF16),
            VMEM((2 * T, 2 * T), F32), VMEM((2 * T, 2 * T), F32), VMEM((HEAD, 2 * T), F32),
            DMA((3,)), DMA((3,)), DMA((3,)), DMA((10,)), DMA((10,)),
            DMA((11, cp)), DMA((11, cp)), DMA((11, cp)), DMA((11, cp)), DMA((11,)),
            DMA((10,)), DMA((10,)), DMA((2 * cp, 2)), DMA((2 * cp, 2)), DMA((2,)),
            DMA((nx,)), DMA((nx,)), DMA((nx, cp)), DMA((nx, cp)),
        ],
        compiler_params=params(0),
        name='attn',
    )(x, wq, wk, wv, wo, idx.T)


def experts(h, prow, gates, w1g, w1u, w2, cp, tp, cap):
    T, H = h.shape
    F = w1g.shape[2]
    ne = cp * tp
    return pl.pallas_call(
        functools.partial(moe_kernel, cp, tp, cap),
        out_shape=jax.ShapeDtypeStruct((T, H), BF16),
        in_specs=[spec(VMEM)] * 3 + [spec(pl.ANY)] * 3,
        out_specs=spec(VMEM),
        scratch_shapes=[VMEM((ne, cap, H), BF16)] * 4 + [
            VMEM((H, F), BF16), VMEM((H, F), BF16), VMEM((F, H), BF16), VMEM((T, H), F32), VMEM((T, HEAD), F32),
            DMA((3,)), DMA((ne,)), DMA((ne,)), DMA((ne,)), DMA((ne,)),
        ],
        compiler_params=params(1),
        name='moe',
    )(h, prow, gates.T, w1g, w1u, w2)


def solution(mesh):
    cp = mesh.shape['cp']
    tp = mesh.shape['tp']
    rows_spec = P(('dp', 'cp', 'tp'), None)
    exp_spec = P(('cp', 'tp'), None, None)

    def local(x, idx, gates, wq, wk, wv, wo, w1g, w1u, w2):
        cap = 4 * x.shape[0] // (cp * tp)
        h, prow = attention(x, idx, wq, wk, wv, wo, cp, tp, cap)
        return experts(h, prow, gates, w1g, w1u, w2, cp, tp, cap)

    return jax.shard_map(local, mesh=mesh, in_specs=(rows_spec, rows_spec, rows_spec, P(None, 'tp'), P(None, 'tp'), P(None, 'tp'), P('tp', None), exp_spec, exp_spec, exp_spec), out_specs=rows_spec, check_vma=False)
```
